256 devices in a mesh: gx: 4 (over z_lo), gy: 8 (over x, core), tracer: 8 (over z_hi, y).
Axes of the slice: x: 4, y: 4, z: 8 (z_hi: 2, z_lo: 4; z = z_hi * 4 + z_lo), core: 2. Of those that a mesh axis runs over, the one named last changes fastest.
Arguments:
- biology_concentration: float32 [24, 8, 512, 512], P('tracer', None, 'gy', 'gx'), may hold values from 0.1 to 2
- flow_vectors: float32 [2, 8, 512, 512], P(None, 'tracer', 'gy', 'gx'), may hold values from -0.25 to 0.25
- thermal_anomaly: float32 [8, 512, 512], P('tracer', 'gy', 'gx'), may hold values from -6 to 6
- diffusivity_profile: float32 [8, 512, 512], P(None, 'gy', 'gx'), may hold values from 0.02 to 0.24
- solar_flux_field: float32 [512, 512], P('gy', 'gx'), may hold values from 0.5 to 2
- ecosystem_coefficients: float32 [24], P('tracer'), may hold values from 0.05 to 0.5
- ocean_indicator: int32 [512, 512], P('gy', 'gx'), may hold values 0 or 1
- floor_tier_number: int32 [512, 512], P('gy', 'gx'), may hold values from 1 to 8
Outputs:
- tracers_out: float32 [24, 8, 512, 512], P('tracer', None, 'gy', 'gx')
- currents_out: float32 [2, 8, 512, 512], P(None, 'tracer', 'gy', 'gx')
- temperature_out: float32 [8, 512, 512], P('tracer', 'gy', 'gx')
The draws below stay inside these ranges and needn't reach their ends.
All inputs are finite; a program needn't handle non-finite values. No bound on the sum of `ocean_indicator` on one device may be relied on, other than what follows from the above.
Results may differ from the reference program's by a relative error of at most 0.0003.
Values sent between devices are 32-bit elements; how exact they have to be, the bound alone decides.
No kernel may reach another device: no remote copies, remote signals or barrier semaphores. Data moves between devices by JAX's collectives and lax.ppermute only.
A program may use at most 64 MiB of HBM per device.

```python
import math
import jax
import jax.numpy as jnp

NTR = 24
VERTICAL_TIERS = 8
STEPS = 2
MESH_LONGITUDES = 512
MESH_LATITUDES = 512


def set_ends(entries, rng, low, high):
    spot = [jax.random.randint(jax.random.fold_in(rng, axis), (), 0, length) for axis, length in enumerate(entries.shape)]
    widest = entries.shape.index(max(entries.shape))
    neighbour = spot[:widest] + [(spot[widest] + 1) % entries.shape[widest]] + spot[widest + 1:]
    return entries.at[tuple(spot)].set(low).at[tuple(neighbour)].set(high)


def block_scale(stream_key, extent, pieces, least, high):
    loudness, own = 1.0, jax.random.fold_in(stream_key, 6)
    for position, blocks in pieces:
        steps = jnp.exp(jax.random.uniform(jax.random.fold_in(own, position), (blocks,), jnp.float32, least / len(pieces), high / len(pieces)))
        loudness = loudness * jnp.repeat(steps, extent[position] // blocks).reshape([-1 if axis == position else 1 for axis in range(len(extent))])
    return loudness


def noise(stream_key, extent, width, bound, shards=(), kind=jnp.bfloat16):
    factor_of = block_scale(stream_key, extent, shards, -0.22, 0.18) if shards else 1.0
    values = jax.random.normal(stream_key, extent, jnp.float32) * width * factor_of
    return jnp.minimum(jnp.maximum(values, -bound), bound).astype(kind)


def setup_inputs(seed: int = 0) -> dict:
    seeds = jax.random.split(jax.random.key(seed), 9)
    return {
        "biology_concentration": jnp.clip(jnp.exp(math.log(2.0) - 2.9957323 * jax.random.uniform(seeds[0], (NTR, VERTICAL_TIERS, MESH_LATITUDES, MESH_LONGITUDES), jnp.float32) ** block_scale(seeds[0], (NTR, VERTICAL_TIERS, MESH_LATITUDES, MESH_LONGITUDES), ((0, 8), (2, 8), (3, 4)), -0.2, 0.2)), 0.1, 2.0),
        "flow_vectors": jnp.clip(jax.random.uniform(seeds[1], (2, VERTICAL_TIERS, MESH_LATITUDES, MESH_LONGITUDES), jnp.float32, -0.25, 0.25) * block_scale(seeds[1], (2, VERTICAL_TIERS, MESH_LATITUDES, MESH_LONGITUDES), ((1, 8), (2, 8), (3, 4)), -0.4, 0.0), -0.25, 0.25),
        "thermal_anomaly": noise(seeds[2], (VERTICAL_TIERS, MESH_LATITUDES, MESH_LONGITUDES), 1.0, 6.0, ((0, 8), (1, 8), (2, 4)), jnp.float32),
        "diffusivity_profile": jnp.clip(jnp.exp(math.log(0.24) - 2.4849066 * jax.random.uniform(seeds[3], (VERTICAL_TIERS, MESH_LATITUDES, MESH_LONGITUDES), jnp.float32) ** block_scale(seeds[3], (VERTICAL_TIERS, MESH_LATITUDES, MESH_LONGITUDES), ((1, 8), (2, 4)), -0.2, 0.2)), 0.02, 0.24),
        "solar_flux_field": jnp.clip(jnp.exp(math.log(2.0) - 1.3862944 * jax.random.uniform(seeds[4], (MESH_LATITUDES, MESH_LONGITUDES), jnp.float32) ** block_scale(seeds[4], (MESH_LATITUDES, MESH_LONGITUDES), ((0, 8), (1, 4)), -0.2, 0.2)), 0.5, 2.0),
        "ecosystem_coefficients": jnp.clip(jnp.exp(math.log(0.5) - 2.3025851 * jax.random.uniform(seeds[5], (NTR,), jnp.float32) ** block_scale(seeds[5], (NTR,), ((0, 8),), -0.2, 0.2)), 0.05, 0.5),
        "ocean_indicator": set_ends((jax.random.randint(seeds[6], (MESH_LATITUDES, MESH_LONGITUDES), 0, 10) < 9).astype(jnp.int32), jax.random.fold_in(seeds[6], 1), 0, 1),
        "floor_tier_number": set_ends(jax.random.randint(seeds[7], (MESH_LATITUDES, MESH_LONGITUDES), 1, VERTICAL_TIERS + 1), jax.random.fold_in(seeds[7], 1), 1, VERTICAL_TIERS).astype(jnp.int32),
    }


viscosity = 0.2
water_absorb = 0.04
plankton_absorb = 0.03
heat_share = 0.5
light_half = 0.3
nutrient_half = 0.5


def to_east(values):
    return jnp.concatenate([values[..., 1:], jnp.zeros_like(values[..., :1])], -1)


def to_west(values):
    return jnp.concatenate([jnp.zeros_like(values[..., :1]), values[..., :-1]], -1)


def to_north(values):
    return jnp.concatenate([values[..., 1:, :], jnp.zeros_like(values[..., :1, :])], -2)


def to_south(values):
    return jnp.concatenate([jnp.zeros_like(values[..., :1, :]), values[..., :-1, :]], -2)


def laplace_of(values):
    return to_east(values) + to_west(values) + to_north(values) + to_south(values) - 4.0 * values


def minmod(former, latter):
    return 0.5 * (jnp.sign(former) + jnp.sign(latter)) * jnp.minimum(jnp.abs(former), jnp.abs(latter))


def limited(behind, center, ahead_one, beyond, velocity):
    slope_mid = ahead_one - center
    forward = velocity * (center + 0.5 * (1.0 - velocity) * minmod(slope_mid, center - behind))
    backward = velocity * (ahead_one - 0.5 * (1.0 + velocity) * minmod(slope_mid, beyond - ahead_one))
    return jnp.where(velocity >= 0.0, forward, backward)


def advect_padded(padded, east_pad, north_pad):
    water_span_tiers = padded.shape[-2] - 4
    width_cells = padded.shape[-1] - 4
    row_band = padded[..., 2:water_span_tiers + 2, :]
    flux_x = limited(row_band[..., 0:width_cells + 1], row_band[..., 1:width_cells + 2],
                     row_band[..., 2:width_cells + 3], row_band[..., 3:width_cells + 4],
                     east_pad[:, 2:water_span_tiers + 2, 1:width_cells + 2])
    col_band = padded[..., 2:width_cells + 2]
    flux_y = limited(col_band[..., 0:water_span_tiers + 1, :], col_band[..., 1:water_span_tiers + 2, :],
                     col_band[..., 2:water_span_tiers + 3, :], col_band[..., 3:water_span_tiers + 4, :],
                     north_pad[:, 1:water_span_tiers + 2, 2:width_cells + 2])
    inner_cells = padded[..., 2:water_span_tiers + 2, 2:width_cells + 2]
    return inner_cells - (flux_x[..., 1:] - flux_x[..., :-1]) - (flux_y[..., 1:, :] - flux_y[..., :-1, :])


def vertical_mix(tracer_field, coupling):
    level_below = jnp.concatenate([tracer_field[:, 1:], jnp.zeros_like(tracer_field[:, :1])], 1)
    level_above = jnp.concatenate([jnp.zeros_like(tracer_field[:, :1]), tracer_field[:, :-1]], 1)
    coupling_above = jnp.concatenate([jnp.zeros_like(coupling[:1]), coupling[:-1]], 0)
    return tracer_field + coupling * (level_below - tracer_field) - coupling_above * (tracer_field - level_above)


def light_fields(absorb, solar_flux_field):
    attenuation = water_absorb + plankton_absorb * absorb
    depth_top = jnp.cumsum(attenuation, 0) - attenuation
    light_mid = solar_flux_field * jnp.exp(-depth_top - 0.5 * attenuation)
    heating = heat_share * solar_flux_field * (jnp.exp(-depth_top) - jnp.exp(-depth_top - attenuation))
    return light_mid, heating


def biology(tracer_field, light_mid, rate_values, wet_full):
    tracer_count = tracer_field.shape[0]
    triples = tracer_field.reshape((tracer_count // 3, 3) + tracer_field.shape[1:])
    rate_sets = rate_values.reshape(tracer_count // 3, 3)
    nutrient, plankton, detritus = triples[:, 0], triples[:, 1], triples[:, 2]
    growth = rate_sets[:, 0][:, None, None, None]
    mortal = rate_sets[:, 1][:, None, None, None]
    recycle_rate = rate_sets[:, 2][:, None, None, None]
    uptake = growth * (light_mid / (light_mid + light_half)) * plankton * nutrient / (jnp.abs(nutrient) + nutrient_half)
    mortality = mortal * plankton
    recycled = recycle_rate * detritus
    result = jnp.stack([nutrient - uptake + recycled, plankton + uptake - mortality, detritus + mortality - recycled], 1)
    return result.reshape(tracer_field.shape) * wet_full


def reference(biology_concentration, flow_vectors, thermal_anomaly, diffusivity_profile, solar_flux_field, ecosystem_coefficients, ocean_indicator, floor_tier_number):
    depth_index = jnp.arange(VERTICAL_TIERS, dtype=jnp.int32)[:, None, None]
    wet_full = (ocean_indicator[None] * (depth_index < floor_tier_number[None]).astype(jnp.int32)).astype(jnp.float32)
    open_east = wet_full * to_east(wet_full)
    open_north = wet_full * to_north(wet_full)
    coriolis = (0.1 + 0.1 * jnp.arange(MESH_LATITUDES, dtype=jnp.float32) / MESH_LATITUDES)[:, None]
    wet_below = jnp.concatenate([wet_full[1:], jnp.zeros_like(wet_full[:1])], 0)
    coupling = diffusivity_profile * wet_full * wet_below
    tracer_field = biology_concentration
    east_flow = flow_vectors[0]
    north_flow = flow_vectors[1]
    warming_forcing = thermal_anomaly
    padding = ((0, 0), (0, 0), (2, 2), (2, 2))
    for repeat in range(STEPS):
        east_flux = open_east * east_flow
        north_flux = open_north * north_flow
        next_east = open_east * (east_flow + coriolis * north_flow + viscosity * laplace_of(east_flow))
        next_north = open_north * (north_flow - coriolis * east_flow + viscosity * laplace_of(north_flow))
        padded = jnp.pad(tracer_field, padding)
        east_pad = jnp.pad(east_flux, padding[1:])
        north_pad = jnp.pad(north_flux, padding[1:])
        tracer_field = advect_padded(padded, east_pad, north_pad) * wet_full
        tracer_field = vertical_mix(tracer_field, coupling)
        absorb = jnp.sum(tracer_field[1::3], 0)
        light_mid, heating = light_fields(absorb, solar_flux_field)
        tracer_field = biology(tracer_field, light_mid, ecosystem_coefficients, wet_full)
        eastward = jnp.maximum(east_flux, 0.0) * warming_forcing + jnp.minimum(east_flux, 0.0) * to_east(warming_forcing)
        northward = jnp.maximum(north_flux, 0.0) * warming_forcing + jnp.minimum(north_flux, 0.0) * to_north(warming_forcing)
        warming_forcing = wet_full * (warming_forcing - eastward + to_west(eastward) - northward + to_south(northward) + heating)
        east_flow, north_flow = next_east, next_north
    return tracer_field, jnp.stack([east_flow, north_flow]), warming_forcing
```

```python
import jax
import jax.numpy as jnp
from jax import lax
from jax.experimental import pallas as pl
from jax.experimental.pallas import tpu as pltpu
from jax.sharding import PartitionSpec as P

NL = 8
R = 64
W = 128
NT = 3
NCH = NT * NL
HY = 16
f32 = jnp.float32
VM = pl.BlockSpec(memory_space=pltpu.VMEM)
SM = pl.BlockSpec(memory_space=pltpu.SMEM)


def call(body, name, outs, n_scalar, scratch=()):
    def run(*args):
        return pl.pallas_call(
            body,
            name=name,
            out_shape=[jax.ShapeDtypeStruct(s, f32) for s in outs],
            in_specs=[SM] * n_scalar + [VM] * (len(args) - n_scalar),
            out_specs=[VM] * len(outs),
            scratch_shapes=[pltpu.VMEM(s, f32) for s in scratch],
            compiler_params=pltpu.CompilerParams(vmem_limit_bytes=40 * 2**20),
        )(*args)

    return run


def lanes(shape):
    return lax.broadcasted_iota(jnp.int32, shape, 1)


def rx(v, k):
    return pltpu.roll(v, k % v.shape[1], 1)


def ry(v, k):
    return pltpu.roll(v, k % v.shape[0], 0)


def aside(v, shift):
    return pltpu.roll(v, shift, 1)


def minmod(a, b):
    return jnp.maximum(jnp.minimum(a, b), 0.0) + jnp.minimum(jnp.maximum(a, b), 0.0)


def coefs(vel):
    up = jnp.maximum(vel, 0.0)
    um = jnp.minimum(vel, 0.0)
    return up, um, 0.5 * up * (1.0 - up), 0.5 * um * (1.0 + um)


def divergence(c, co, roll):
    up, um, a, b = co
    ahead = roll(c, -1)
    d = ahead - c
    s = minmod(d, roll(d, 1))
    flux = up * c + a * s + um * ahead - b * roll(s, -1)
    return flux - roll(flux, 1)


def upwind(c, vel, roll):
    flux = jnp.maximum(vel, 0.0) * c + jnp.minimum(vel, 0.0) * roll(c, -1)
    return flux - roll(flux, 1)


def put_x(acc, value, lane, width):
    at = lanes(acc.shape)
    half = width // 2
    return jnp.where((at >= lane) & (at < lane + width), pltpu.roll(value, lane + half, 1), acc)


def pack_tracers(c_ref, px_ref, pyu_ref, pyd_ref):
    def level(l, carry):
        for t in range(NT):
            ch = t * NL + l
            c = c_ref[t, l]
            px_ref[...] = put_x(px_ref[...], c, 4 * ch, 4)
            pyu_ref[pl.ds(2 * ch, 2), :] = c_ref[t, l, R - 2 : R, :]
            pyd_ref[pl.ds(2 * ch, 2), :] = c_ref[t, l, 0:2, :]
        return carry

    lax.fori_loop(0, NL, level, 0)


def pack_rows(value, row, pyu_ref, pyd_ref):
    pyu_ref[row : row + 1, :] = value[R - 1 : R, :]
    pyd_ref[row : row + 1, :] = value[0:1, :]


def first_pack(c_ref, flow_ref, temp_ref, sea_ref, floor_ref, px_ref, pyu_ref, pyd_ref):
    px_ref[...] = jnp.zeros_like(px_ref)
    pyu_ref[...] = jnp.zeros_like(pyu_ref)
    pyd_ref[...] = jnp.zeros_like(pyd_ref)
    pack_tracers(c_ref, px_ref, pyu_ref, pyd_ref)
    singles = (
        flow_ref[0, 0],
        flow_ref[1, 0],
        temp_ref[0],
        sea_ref[...].astype(f32),
        floor_ref[...].astype(f32),
    )
    acc = px_ref[...]
    for j, value in enumerate(singles):
        acc = put_x(acc, value, 96 + 2 * j, 2)
        pack_rows(value, 48 + j, pyu_ref, pyd_ref)
    px_ref[...] = acc


def join_x(ids_ref, even, odd, left_end=96):
    at = lanes(even.shape)
    half = jnp.where(at < 96, (at >> 1) & 1, jnp.where(at < left_end, 0, at & 1))
    return jnp.where(half == (ids_ref[1] & 1), odd, even)


def edges_y(ids_ref, lo_ref, hi_ref, los_ref, his_ref):
    gy = ids_ref[2]
    los_ref[...] = jnp.where(gy == 0, 0.0, lo_ref[...])
    his_ref[...] = jnp.where(gy == ids_ref[3] - 1, 0.0, hi_ref[...])


def extend_flow(ids_ref, flow_ref, even_ref, odd_ref, lo_ref, hi_ref, e_ref):
    joined = join_x(ids_ref, even_ref[...], odd_ref[...])
    padded = jnp.concatenate([joined, jnp.zeros_like(joined)], 0)
    turned = padded.T
    gy = ids_ref[2]
    e_ref[0:R, :] = flow_ref[0, 0]
    e_ref[R : 2 * R, :] = flow_ref[1, 0]
    e_ref[2 * R : 2 * R + 4, :] = turned[96:100, :]
    lo = jnp.where(gy == 0, 0.0, lo_ref[48:50, :])
    hi = jnp.where(gy == ids_ref[3] - 1, 0.0, hi_ref[48:50, :])
    e_ref[2 * R + 4 : 2 * R + 6, :] = lo
    e_ref[2 * R + 6 : 2 * R + 8, :] = hi


def wet_setup(xh, los_ref, his_ref, sea_ref, floor_ref, wx_ref, wy_ref):
    for k, ref in enumerate((sea_ref, floor_ref)):
        main = ref[...].astype(f32)
        wx_ref[k, :, :W] = main
        wx_ref[k, :, W:] = aside(xh, (127 - (96 + 2 * (3 + k))) % W)
        wy_ref[k, :R, :] = main
        wy_ref[k, R : R + HY, :] = jnp.zeros((HY, W), f32)
        wy_ref[k, R : R + 1, :] = his_ref[51 + k : 52 + k, :]
        wy_ref[k, R + HY - 1 : R + HY, :] = los_ref[51 + k : 52 + k, :]


def wet_of(ref, l):
    return jnp.where(l.astype(f32) < ref[1], ref[0], 0.0)


def advect_level(l, c_ref, xh_ref, los_ref, his_ref, east, north, wet, cy_ref, adv_ref):
    east_co = coefs(east)
    north_co = coefs(north)
    for t in range(NT):
        ch = t * NL + l
        c = c_ref[t, l]
        cx = jnp.concatenate([c, aside(xh_ref[...], lax.rem(126 + W - 4 * ch, W))], 1)
        div = divergence(cx, east_co, rx)[:, :W]
        cy_ref[t, 0:R, :] = c
        cy_ref[t, R : R + 2, :] = his_ref[pl.ds(2 * ch, 2), :]
        cy_ref[t, R + HY - 2 : R + HY, :] = los_ref[pl.ds(2 * ch, 2), :]
        div = div + divergence(cy_ref[t], north_co, ry)[:R]
        adv_ref[t, l] = wet * (c - div)


def mix(adv_ref, dif_ref, wx_ref, mix_ref):
    above = None
    wet = wet_of(wx_ref, jnp.int32(0))[:, :W]
    for l in range(NL):
        if l + 1 < NL:
            below_wet = wet_of(wx_ref, jnp.int32(l + 1))[:, :W]
            below = dif_ref[l] * wet * below_wet
        for t in range(NT):
            c = adv_ref[t, l]
            out = c
            if l + 1 < NL:
                out = out + below * (adv_ref[t, l + 1] - c)
            if l:
                out = out - above * (c - adv_ref[t, l - 1])
            mix_ref[t, l] = out
        above, wet = below, below_wet


def split_absorb(ids_ref, mix_ref, parts):
    y = ids_ref[0] & 3
    for k, ref in enumerate(parts):
        j = (y + k) & 3
        ref[...] = mix_ref[1, pl.ds(2 * j, 2)]


def next_currents(u, v, ux, uy, vx, vy, east_open, north_open, coriolis):
    lap_u = (rx(ux, -1) + rx(ux, 1))[:, :W] + (ry(uy, -1) + ry(uy, 1))[:R] - 4.0 * u
    lap_v = (rx(vx, -1) + rx(vx, 1))[:, :W] + (ry(vy, -1) + ry(vy, 1))[:R] - 4.0 * v
    return (
        east_open * (u + coriolis * v + 0.2 * lap_u),
        north_open * (v - coriolis * u + 0.2 * lap_v),
    )


def coriolis_of(ids_ref):
    row = ids_ref[2] * R + lax.broadcasted_iota(jnp.int32, (R, W), 0)
    rows = (ids_ref[3] * R).astype(f32)
    return 0.1 + 0.1 * row.astype(f32) / rows


def with_y(ref, main, hi, lo):
    ref[0:R, :] = main
    ref[R : R + 1, :] = hi
    ref[R + HY - 1 : R + HY, :] = lo
    return ref[...]


def open_x(wx):
    return wx * rx(wx, -1)


def open_y(wy):
    return wy * ry(wy, -1)


def step_one(
    ids_ref, c_ref, g0, g1, g2, g3, even_ref, odd_ref, lo_ref, hi_ref, temp_ref, dif_ref, sea_ref,
    floor_ref, mix_ref, a0, a1, a2, a3, cur_ref, tadv_ref,
    g_ref, xh_ref, los_ref, his_ref, wx_ref, wy_ref, cy_ref, adv_ref, gx_ref, uy_ref,
):
    y = ids_ref[0] & 3
    z = ids_ref[0] >> 2
    for k, ref in enumerate((g0, g1, g2, g3)):
        for zz in range(2):
            g_ref[((z + zz) & 1) * 4 + ((y + 4 - k) & 3)] = ref[zz]
    xh = join_x(ids_ref, even_ref[...], odd_ref[...])
    xh_ref[...] = xh
    edges_y(ids_ref, lo_ref, hi_ref, los_ref, his_ref)
    wet_setup(xh, los_ref, his_ref, sea_ref, floor_ref, wx_ref, wy_ref)
    cols = jnp.concatenate([g_ref[l, 2 * R : 2 * R + 8, :] for l in range(NL)], 0)
    gx_ref[...] = jnp.concatenate([cols, jnp.zeros_like(cols)], 0).T[:R, :]
    coriolis = coriolis_of(ids_ref)

    def faces(l):
        u = g_ref[l, 0:R, :]
        v = g_ref[l, R : 2 * R, :]
        ux = jnp.concatenate([u, aside(gx_ref[...], lax.rem(W + 127 - 8 * l, W))], 1)
        edge = 2 * R + 4
        vy = with_y(
            uy_ref.at[1], v, g_ref[l, edge + 3 : edge + 4, :], g_ref[l, edge + 1 : edge + 2, :]
        )
        wx = wet_of(wx_ref, l)
        east_open = open_x(wx)
        north_open = open_y(wet_of(wy_ref, l))
        return u, v, ux, vy, wx, east_open, north_open

    def level(l, carry):
        u, v, ux, vy, wx, east_open, north_open = faces(l)
        vx = jnp.concatenate([v, aside(gx_ref[...], lax.rem(W + 125 - 8 * l, W))], 1)
        edge = 2 * R + 4
        uy = with_y(
            uy_ref.at[0], u, g_ref[l, edge + 2 : edge + 3, :], g_ref[l, edge : edge + 1, :]
        )
        new_u, new_v = next_currents(
            u, v, ux, uy, vx, vy, east_open[:, :W], north_open[:R], coriolis
        )
        cur_ref[0, l] = new_u
        cur_ref[1, l] = new_v
        advect_level(
            l, c_ref, xh_ref, los_ref, his_ref, east_open * ux, north_open * vy, wx[:, :W],
            cy_ref, adv_ref,
        )
        return carry

    lax.fori_loop(0, NL, level, 0)
    mix(adv_ref, dif_ref, wx_ref, mix_ref)
    split_absorb(ids_ref, mix_ref, (a0, a1, a2, a3))
    u, v, ux, vy, wx, east_open, north_open = faces(ids_ref[0])
    temp = temp_ref[0]
    tx = jnp.concatenate([temp, aside(xh_ref[...], 127 - 100)], 1)
    ty = with_y(uy_ref.at[0], temp, his_ref[50:51, :], los_ref[50:51, :])
    tadv_ref[...] = (
        temp - upwind(tx, east_open * ux, rx)[:, :W] - upwind(ty, north_open * vy, ry)[:R]
    )


def step_two(
    ids_ref, c_ref, cur_ref, even_ref, odd_ref, lo_ref, hi_ref, even1_ref, odd1_ref, lo1_ref,
    hi1_ref, temp_ref, dif_ref, sea_ref, floor_ref, mix_ref, a0, a1, a2, a3, out_ref, tadv_ref,
    xh_ref, los_ref, his_ref, wx_ref, wy_ref, cy_ref, adv_ref, uy_ref,
):
    xh1 = join_x(ids_ref, even1_ref[...], odd1_ref[...])
    edges_y(ids_ref, lo1_ref, hi1_ref, los_ref, his_ref)
    wet_setup(xh1, los_ref, his_ref, sea_ref, floor_ref, wx_ref, wy_ref)
    xh_ref[...] = join_x(ids_ref, even_ref[...], odd_ref[...], 104)
    edges_y(ids_ref, lo_ref, hi_ref, los_ref, his_ref)

    def faces(l):
        u = cur_ref[0, l]
        v = cur_ref[1, l]
        ux = jnp.concatenate([u, aside(xh_ref[...], 31 - l)], 1)
        vlow = los_ref[pl.ds(48 + l, 1), :]
        vy = with_y(uy_ref.at[1], v, vlow, vlow)
        wx = wet_of(wx_ref, l)
        return u, v, ux, vy, wx, open_x(wx), open_y(wet_of(wy_ref, l))

    def level(l, carry):
        u, v, ux, vy, wx, east_open, north_open = faces(l)
        advect_level(
            l, c_ref, xh_ref, los_ref, his_ref, east_open * ux, north_open * vy, wx[:, :W],
            cy_ref, adv_ref,
        )
        return carry

    lax.fori_loop(0, NL, level, 0)
    mix(adv_ref, dif_ref, wx_ref, mix_ref)
    split_absorb(ids_ref, mix_ref, (a0, a1, a2, a3))
    u, v, ux, vy, wx, east_open, north_open = faces(ids_ref[0])
    temp = temp_ref[...]
    tx = jnp.concatenate([temp, aside(xh_ref[...], 127 - 108)], 1)
    ty = with_y(uy_ref.at[0], temp, his_ref[58:59, :], los_ref[58:59, :])
    tadv_ref[...] = (
        temp - upwind(tx, east_open * ux, rx)[:, :W] - upwind(ty, north_open * vy, ry)[:R]
    )
    ux = jnp.concatenate([u, aside(xh_ref[...], 127 - 104)], 1)
    vx = jnp.concatenate([v, aside(xh_ref[...], 127 - 106)], 1)
    uy = with_y(uy_ref.at[0], u, his_ref[56:57, :], los_ref[56:57, :])
    vy = with_y(uy_ref.at[1], v, his_ref[57:58, :], los_ref[57:58, :])
    new_u, new_v = next_currents(
        u, v, ux, uy, vx, vy, east_open[:, :W], north_open[:R], coriolis_of(ids_ref)
    )
    out_ref[0] = new_u
    out_ref[1] = new_v


def biology(ids_ref, rate_ref, mix_ref, parts, solar_ref, sea_ref, floor_ref, c_ref, sum_ref, heat_ref):
    y = ids_ref[0] & 3
    for k, ref in enumerate(parts):
        sum_ref[pl.ds(2 * ((y + 4 - k) & 3), 2)] = ref[...]
    solar = solar_ref[...]
    sea = sea_ref[...].astype(f32)
    mu, mortal, recycle = rate_ref[0], rate_ref[1], rate_ref[2]

    def level(l, tau):
        a = 0.04 + 0.03 * sum_ref[l]
        light = solar * jnp.exp(-tau - 0.5 * a)
        heat_ref[l] = 0.5 * solar * (jnp.exp(-tau) - jnp.exp(-tau - a))
        wet = jnp.where(l < floor_ref[...], sea, 0.0)
        n, p, d = mix_ref[0, l], mix_ref[1, l], mix_ref[2, l]
        uptake = mu * (light / (light + 0.3)) * p * n / (jnp.abs(n) + 0.5)
        dead = mortal * p
        back = recycle * d
        c_ref[0, l] = wet * (n - uptake + back)
        c_ref[1, l] = wet * (p + uptake - dead)
        c_ref[2, l] = wet * (d + dead - back)
        return tau + a

    lax.fori_loop(0, NL, level, jnp.zeros((R, W), f32))
    own = ids_ref[0]
    wet = jnp.where(own < floor_ref[...], sea, 0.0)
    return heat_ref[own], wet


def biology_pack(
    ids_ref, rate_ref, mix_ref, t0, t1, t2, t3, solar_ref, sea_ref, floor_ref, tadv_ref, cur_ref,
    c_ref, temp_ref, px_ref, pyu_ref, pyd_ref, sum_ref, heat_ref,
):
    heat, wet = biology(
        ids_ref, rate_ref, mix_ref, (t0, t1, t2, t3), solar_ref, sea_ref, floor_ref, c_ref,
        sum_ref, heat_ref,
    )
    temp = wet * (tadv_ref[...] + heat)
    temp_ref[...] = temp
    px_ref[...] = jnp.zeros_like(px_ref)
    pyu_ref[...] = jnp.zeros_like(pyu_ref)
    pyd_ref[...] = jnp.zeros_like(pyd_ref)
    pack_tracers(c_ref, px_ref, pyu_ref, pyd_ref)
    acc = px_ref[...]
    at = lanes(acc.shape)
    for l in range(NL):
        acc = jnp.where(at == 96 + l, pltpu.roll(cur_ref[0, l], 97 + l, 1), acc)
        pyu_ref[48 + l : 49 + l, :] = cur_ref[1, l, R - 1 : R, :]
    own = ids_ref[0]
    for j, value in enumerate((cur_ref[0, own], cur_ref[1, own], temp)):
        acc = put_x(acc, value, 104 + 2 * j, 2)
        pack_rows(value, 56 + j, pyu_ref, pyd_ref)
    px_ref[...] = acc


def biology_last(
    ids_ref, rate_ref, mix_ref, t0, t1, t2, t3, solar_ref, sea_ref, floor_ref, tadv_ref,
    c_ref, temp_ref, sum_ref, heat_ref,
):
    heat, wet = biology(
        ids_ref, rate_ref, mix_ref, (t0, t1, t2, t3), solar_ref, sea_ref, floor_ref, c_ref,
        sum_ref, heat_ref,
    )
    temp_ref[0] = wet * (tadv_ref[...] + heat)


def swap_pairs(value, axis):
    n = lax.axis_size(axis)
    even = [(i, j) for a in range(0, n - 1, 2) for i, j in ((a, a + 1), (a + 1, a))]
    odd = [(i, j) for a in range(1, n - 1, 2) for i, j in ((a, a + 1), (a + 1, a))]
    return lax.ppermute(value, axis, even), lax.ppermute(value, axis, odd)


def ring_y(up, down):
    n = lax.axis_size("gy")
    ahead = [(i, (i + 1) % n) for i in range(n)]
    back = [(b, a) for a, b in ahead]
    return lax.ppermute(up, "gy", ahead), lax.ppermute(down, "gy", back)


def by_y(k):
    return [(z * 4 + y, z * 4 + (y + k) % 4) for z in range(2) for y in range(4)]


def over_z(value):
    return lax.ppermute(value, "tracer", [(i, i ^ 4) for i in range(8)])


def spread_y(value):
    return [value] + [lax.ppermute(value, "tracer", by_y(k)) for k in (1, 2, 3)]


def total(parts):
    got = [parts[0]] + [lax.ppermute(parts[k], "tracer", by_y(k)) for k in (1, 2, 3)]
    mine = got[0] + got[1] + (got[2] + got[3])
    return spread_y(mine + over_z(mine))


def per_device(c, flow, temp, dif, solar, rates, sea, floor):
    ids = jnp.stack(
        [
            lax.axis_index("tracer"),
            lax.axis_index("gx"),
            lax.axis_index("gy"),
            jnp.int32(lax.axis_size("gy")),
        ]
    )
    tile = (R, W)
    full = (NT, NL, R, W)
    part = (2, R, W)
    px, pyu, pyd = call(first_pack, "pack_one", [tile, tile, tile], 0)(c, flow, temp, sea, floor)
    even, odd = swap_pairs(px, "gx")
    lo, hi = ring_y(pyu, pyd)
    (own,) = call(extend_flow, "extend", [(2 * R + 8, W)], 1)(ids, flow, even, odd, lo, hi)
    gathered = spread_y(jnp.stack([own, over_z(own)]))
    edge = [tile, tile]
    wets = [(2, R, 2 * W), (2, R + HY, W)]
    mixed, a0, a1, a2, a3, cur, tadv = call(
        step_one, "step_one", [full, part, part, part, part, (2, NL, R, W), tile], 1,
        [(NL, 2 * R + 8, W), tile] + edge + wets + [(NT, R + HY, W), full, tile, (2, R + HY, W)],
    )(ids, c, *gathered, even, odd, lo, hi, temp, dif, sea, floor)
    sums = total((a0, a1, a2, a3))
    c, heated, px, pyu, pyd = call(
        biology_pack, "biology_one", [full, tile, tile, tile, tile], 2, [(NL, R, W), (NL, R, W)]
    )(ids, rates, mixed, *sums, solar, sea, floor, tadv, cur)
    even2, odd2 = swap_pairs(px, "gx")
    lo2, hi2 = ring_y(pyu, pyd)
    mixed, a0, a1, a2, a3, currents, tadv = call(
        step_two, "step_two", [full, part, part, part, part, (2, R, W), tile], 1,
        [tile] + edge + wets + [(NT, R + HY, W), full, (2, R + HY, W)],
    )(ids, c, cur, even2, odd2, lo2, hi2, even, odd, lo, hi, heated, dif, sea, floor)
    sums = total((a0, a1, a2, a3))
    c, last_temp = call(
        biology_last, "biology_two", [full, (1, R, W)], 2, [(NL, R, W), (NL, R, W)]
    )(ids, rates, mixed, *sums, solar, sea, floor, tadv)
    return c, currents.reshape(2, 1, R, W), last_temp


def solution(mesh):
    in_specs = (
        P("tracer", None, "gy", "gx"),
        P(None, "tracer", "gy", "gx"),
        P("tracer", "gy", "gx"),
        P(None, "gy", "gx"),
        P("gy", "gx"),
        P("tracer"),
        P("gy", "gx"),
        P("gy", "gx"),
    )
    out_specs = (
        P("tracer", None, "gy", "gx"),
        P(None, "tracer", "gy", "gx"),
        P("tracer", "gy", "gx"),
    )
    return jax.shard_map(
        per_device, mesh=mesh, in_specs=in_specs, out_specs=out_specs, check_vma=False
    )
```

```python
import jax
import jax.numpy as jnp
from jax import lax
from jax.experimental import pallas as pl
from jax.experimental.pallas import tpu as pltpu
from jax.sharding import PartitionSpec as P

NL = 8
R = 64
W = 128
NT = 3
NCH = NT * NL
HY = 16
UNROLL = 4
f32 = jnp.float32
VM = pl.BlockSpec(memory_space=pltpu.VMEM)
AN = pl.BlockSpec(memory_space=pl.ANY)
HB = pl.BlockSpec(memory_space=pltpu.HBM)
SM = pl.BlockSpec(memory_space=pltpu.SMEM)


def call(body, name, outs, n_scalar, scratch=(), n_any=0, sems=0):
    def run(*args):
        return pl.pallas_call(
            body,
            name=name,
            out_shape=[jax.ShapeDtypeStruct(s, f32) for s in outs],
            in_specs=[SM] * n_scalar + [VM] * (len(args) - n_scalar - n_any) + [HB if sems else AN] * n_any,
            out_specs=[VM] * len(outs),
            scratch_shapes=[s if hasattr(s, "dtype") else pltpu.VMEM(s, f32) for s in scratch]
            + ([pltpu.SemaphoreType.DMA((sems,))] if sems else []),
            compiler_params=pltpu.CompilerParams(vmem_limit_bytes=40 * 2**20),
        )(*args)

    return run


def lanes(shape):
    return lax.broadcasted_iota(jnp.int32, shape, 1)


def rx(v, k):
    return pltpu.roll(v, k % v.shape[1], 1)


def ry(v, k):
    return pltpu.roll(v, k % v.shape[0], 0)


def aside(v, shift):
    return pltpu.roll(v, shift, 1)


def minmod(a, b):
    return jnp.maximum(jnp.minimum(a, b), 0.0) + jnp.minimum(jnp.maximum(a, b), 0.0)


def coefs(vel):
    up = jnp.maximum(vel, 0.0)
    um = jnp.minimum(vel, 0.0)
    return up, um, 0.5 * up * (1.0 - up), 0.5 * um * (1.0 + um)


def divergence(c, co, roll):
    up, um, a, b = co
    ahead = roll(c, -1)
    d = ahead - c
    s = minmod(d, roll(d, 1))
    flux = up * c + a * s + um * ahead - b * roll(s, -1)
    return flux - roll(flux, 1)


def upwind(c, vel, roll):
    flux = jnp.maximum(vel, 0.0) * c + jnp.minimum(vel, 0.0) * roll(c, -1)
    return flux - roll(flux, 1)


def put_x(acc, value, lane, width):
    at = lanes(acc.shape)
    half = width // 2
    return jnp.where((at >= lane) & (at < lane + width), pltpu.roll(value, lane + half, 1), acc)


def pack_tracers(c_refs, px_ref, pyu_ref, pyd_ref):
    def level(l, carry):
        for t in range(NT):
            ch = t * NL + l
            c_ref = c_refs[t]
            px_ref[...] = put_x(px_ref[...], c_ref[l], 4 * ch, 4)
            pyu_ref[pl.ds(2 * ch, 2), :] = c_ref[l, R - 2 : R, :]
            pyd_ref[pl.ds(2 * ch, 2), :] = c_ref[l, 0:2, :]
        return carry

    lax.fori_loop(0, NL, level, 0, unroll=2)


def pack_rows(value, row, pyu_ref, pyd_ref):
    pyu_ref[row : row + 1, :] = value[R - 1 : R, :]
    pyd_ref[row : row + 1, :] = value[0:1, :]


def first_pack(
    c_hbm, flow_hbm, temp_hbm, sea_hbm, floor_hbm, px_ref, pyu_ref, pyd_ref,
    c_ref, flow_ref, temp_ref, sea_ref, floor_ref, sems,
):
    pairs = (
        (c_hbm, c_ref), (flow_hbm, flow_ref), (temp_hbm, temp_ref), (sea_hbm, sea_ref),
        (floor_hbm, floor_ref),
    )
    copies = [pltpu.make_async_copy(a, b, sems.at[k]) for k, (a, b) in enumerate(pairs)]
    for copy in copies:
        copy.start()
    px_ref[...] = jnp.zeros_like(px_ref)
    pyu_ref[...] = jnp.zeros_like(pyu_ref)
    pyd_ref[...] = jnp.zeros_like(pyd_ref)
    for copy in copies[1:]:
        copy.wait()
    singles = (
        (0, flow_ref[0, 0]),
        (1, flow_ref[1, 0]),
        (4, temp_ref[0]),
        (5, sea_ref[...].astype(f32)),
        (6, floor_ref[...].astype(f32)),
    )
    acc = px_ref[...]
    for j, value in singles:
        acc = put_x(acc, value, 96 + 2 * j, 2)
        pack_rows(value, 48 + j, pyu_ref, pyd_ref)
    px_ref[...] = acc
    copies[0].wait()
    pack_tracers([c_ref.at[t] for t in range(NT)], px_ref, pyu_ref, pyd_ref)


def pack_other(other_ref, px_in, pyu_in, pyd_in, px_ref, pyu_ref, pyd_ref):
    pyu_ref[...] = pyu_in[...]
    pyd_ref[...] = pyd_in[...]
    acc = px_in[...]
    for j in range(2):
        value = other_ref[j, 0]
        acc = put_x(acc, value, 100 + 2 * j, 2)
        pack_rows(value, 50 + j, pyu_ref, pyd_ref)
    px_ref[...] = acc


def join_x(ids_ref, left, right, left_end=96):
    at = lanes(left.shape)
    half = jnp.where(at < 96, (at >> 1) & 1, jnp.where(at < left_end, 0, at & 1))
    gx = ids_ref[1]
    left = jnp.where(gx == 0, 0.0, left)
    right = jnp.where(gx == ids_ref[4] - 1, 0.0, right)
    return jnp.where(half == 0, left, right)


def edges_y(ids_ref, lo_ref, hi_ref, los_ref, his_ref):
    gy = ids_ref[2]
    los_ref[...] = jnp.where(gy == 0, 0.0, lo_ref[...])
    his_ref[...] = jnp.where(gy == ids_ref[3] - 1, 0.0, hi_ref[...])


def extend_flow(
    ids_ref, flow_ref, other_ref, left_ref, right_ref, lo_ref, hi_ref, e_ref, xh_ref, los_ref,
    his_ref,
):
    joined = join_x(ids_ref, left_ref[...], right_ref[...])
    xh_ref[...] = joined
    edges_y(ids_ref, lo_ref, hi_ref, los_ref, his_ref)
    turned = jnp.concatenate([joined, jnp.zeros_like(joined)], 0).T
    for k, ref in enumerate((flow_ref, other_ref)):
        e_ref[k, 0:R, :] = ref[0, 0]
        e_ref[k, R : 2 * R, :] = ref[1, 0]
        e_ref[k, 2 * R : 2 * R + 4, :] = turned[96 + 4 * k : 100 + 4 * k, :]
        e_ref[k, 2 * R + 4 : 2 * R + 6, :] = los_ref[48 + 2 * k : 50 + 2 * k, :]
        e_ref[k, 2 * R + 6 : 2 * R + 8, :] = his_ref[48 + 2 * k : 50 + 2 * k, :]


def wet_setup(xh_ref, los_ref, his_ref, sea_ref, floor_ref, wx_ref, wy_ref):
    for k, ref in enumerate((sea_ref, floor_ref)):
        main = ref[...].astype(f32)
        wx_ref[k, :, :W] = main
        wx_ref[k, :, W:] = aside(xh_ref[...], (127 - (96 + 2 * (5 + k))) % W)
        wy_ref[k, :R, :] = main
        wy_ref[k, R : R + HY, :] = jnp.zeros((HY, W), f32)
        wy_ref[k, R : R + 1, :] = his_ref[53 + k : 54 + k, :]
        wy_ref[k, R + HY - 1 : R + HY, :] = los_ref[53 + k : 54 + k, :]


def wet_of(ref, l):
    return jnp.where(l.astype(f32) < ref[1], ref[0], 0.0)


def advect_level(t, l, c, xh_ref, los_ref, his_ref, east, north, wet, cy_all):
    cy_ref = cy_all.at[l]
    ch = t * NL + l
    cx = jnp.concatenate([c, aside(xh_ref[...], lax.rem(126 + W - 4 * ch, W))], 1)
    div = divergence(cx, coefs(east), rx)[:, :W]
    cy_ref[0:R, :] = c
    cy_ref[R : R + 2, :] = his_ref[pl.ds(2 * ch, 2), :]
    cy_ref[R + HY - 2 : R + HY, :] = los_ref[pl.ds(2 * ch, 2), :]
    div = div + divergence(cy_ref[...], coefs(north), ry)[:R]
    return wet * (c - div)


def mix(adv_ref, dif_ref, wx_ref, mix_ref):
    above = None
    wet = wet_of(wx_ref, jnp.int32(0))[:, :W]
    for l in range(NL):
        if l + 1 < NL:
            below_wet = wet_of(wx_ref, jnp.int32(l + 1))[:, :W]
            below = dif_ref[l] * wet * below_wet
        c = adv_ref[l]
        out = c
        if l + 1 < NL:
            out = out + below * (adv_ref[l + 1] - c)
        if l:
            out = out - above * (c - adv_ref[l - 1])
        mix_ref[l] = out
        above, wet = below, below_wet


def split_absorb(ids_ref, mix_ref, parts):
    y = ids_ref[0] & 3
    for k, ref in enumerate(parts):
        j = (y + k) & 3
        ref[...] = mix_ref[pl.ds(2 * j, 2)]


def next_currents(u, v, ux, uy, vx, vy, east_open, north_open, coriolis):
    lap_u = (rx(ux, -1) + rx(ux, 1))[:, :W] + (ry(uy, -1) + ry(uy, 1))[:R] - 4.0 * u
    lap_v = (rx(vx, -1) + rx(vx, 1))[:, :W] + (ry(vy, -1) + ry(vy, 1))[:R] - 4.0 * v
    return (
        east_open * (u + coriolis * v + 0.2 * lap_u),
        north_open * (v - coriolis * u + 0.2 * lap_v),
    )


def coriolis_of(ids_ref):
    row = ids_ref[2] * R + lax.broadcasted_iota(jnp.int32, (R, W), 0)
    rows = (ids_ref[3] * R).astype(f32)
    return 0.1 + 0.1 * row.astype(f32) / rows


def with_y(ref, main, hi, lo):
    ref[0:R, :] = main
    ref[R : R + 1, :] = hi
    ref[R + HY - 1 : R + HY, :] = lo
    return ref[...]


def open_x(wx):
    return wx * rx(wx, -1)


def open_y(wy):
    return wy * ry(wy, -1)


EDGE = 2 * R + 4


def plankton_one(
    ids_ref, c_ref, g0, g1, g2, g3, xh_ref, los_ref, his_ref, dif_ref, sea_ref, floor_ref, mix_ref,
    a0, a1, a2, a3, g_ref, gx_ref, east_ref, north_ref, wx_ref, wy_ref, cy_ref, adv_ref, vy_ref,
):
    y = ids_ref[0] & 3
    z = ids_ref[0] >> 2
    for k, ref in enumerate((g0, g1, g2, g3)):
        for zz in range(2):
            g_ref[((z + zz) & 1) * 4 + ((y + 4 - k) & 3)] = ref[zz]
    wet_setup(xh_ref, los_ref, his_ref, sea_ref, floor_ref, wx_ref, wy_ref)
    cols = jnp.concatenate([g_ref[l, 2 * R : 2 * R + 8, :] for l in range(NL)], 0)
    gx_ref[...] = jnp.concatenate([cols, jnp.zeros_like(cols)], 0).T[:R, :]

    def level(l, carry):
        u = g_ref[l, 0:R, :]
        v = g_ref[l, R : 2 * R, :]
        ux = jnp.concatenate([u, aside(gx_ref[...], lax.rem(W + 127 - 8 * l, W))], 1)
        vy = with_y(vy_ref.at[l], v, g_ref[l, EDGE + 3 : EDGE + 4, :], g_ref[l, EDGE + 1 : EDGE + 2, :])
        wx = wet_of(wx_ref, l)
        east = open_x(wx) * ux
        north = open_y(wet_of(wy_ref, l)) * vy
        east_ref[l] = east
        north_ref[l] = north
        adv_ref[l] = advect_level(
            1, l, c_ref[1, l], xh_ref, los_ref, his_ref, east, north, wx[:, :W], cy_ref
        )
        return carry

    lax.fori_loop(0, NL, level, 0, unroll=UNROLL)
    mix(adv_ref, dif_ref, wx_ref, mix_ref)
    split_absorb(ids_ref, mix_ref, (a0, a1, a2, a3))


def plankton_two(
    ids_ref, c_ref, cur_ref, left_ref, right_ref, lo_ref, hi_ref, dif_ref, wx_ref, wy_ref, mix_ref,
    a0, a1, a2, a3, xh_ref, los_ref, his_ref, east_ref, north_ref, cy_ref, adv_ref, vy_ref,
):
    xh_ref[...] = join_x(ids_ref, left_ref[...], right_ref[...], 104)
    edges_y(ids_ref, lo_ref, hi_ref, los_ref, his_ref)

    def level(l, carry):
        ux = jnp.concatenate([cur_ref[0, l], aside(xh_ref[...], 31 - l)], 1)
        vlow = los_ref[pl.ds(48 + l, 1), :]
        vy = with_y(vy_ref.at[l], cur_ref[1, l], vlow, vlow)
        wx = wet_of(wx_ref, l)
        east = open_x(wx) * ux
        north = open_y(wet_of(wy_ref, l)) * vy
        east_ref[l] = east
        north_ref[l] = north
        adv_ref[l] = advect_level(
            1, l, c_ref[l], xh_ref, los_ref, his_ref, east, north, wx[:, :W], cy_ref
        )
        return carry

    lax.fori_loop(0, NL, level, 0, unroll=UNROLL)
    mix(adv_ref, dif_ref, wx_ref, mix_ref)
    split_absorb(ids_ref, mix_ref, (a0, a1, a2, a3))


def other_tracer(t):
    def body(
        c_ref, xh_ref, los_ref, his_ref, east_ref, north_ref, dif_ref, wx_ref, mix_ref, cy_ref,
        adv_ref,
    ):
        c_ref = c_ref.at[t] if len(c_ref.shape) == 4 else c_ref

        def level(l, carry):
            adv_ref[l] = advect_level(
                t, l, c_ref[l], xh_ref, los_ref, his_ref, east_ref[l], north_ref[l],
                wet_of(wx_ref, l)[:, :W], cy_ref,
            )
            return carry

        lax.fori_loop(0, NL, level, 0, unroll=UNROLL)
        mix(adv_ref, dif_ref, wx_ref, mix_ref)

    return body


def rest_one(
    ids_ref, rate_ref, g_ref, gx_ref, east_ref, north_ref, wx_ref, wy_ref, temp_ref, xh_ref, los_ref, his_ref,
    solar_ref, cur_ref, tadv_ref, sun_ref, pace_ref, ty_ref,
):
    sun_ref[...] = solar_ref[...]
    for t in range(NT):
        pace_ref[t] = jnp.full((8, W), rate_ref[t], f32)
    coriolis = coriolis_of(ids_ref)

    def level(l, carry):
        u = g_ref[l, 0:R, :]
        v = g_ref[l, R : 2 * R, :]
        ux = jnp.concatenate([u, aside(gx_ref[...], lax.rem(W + 127 - 8 * l, W))], 1)
        vx = jnp.concatenate([v, aside(gx_ref[...], lax.rem(W + 125 - 8 * l, W))], 1)
        uy = with_y(
            ty_ref.at[l, 0], u, g_ref[l, EDGE + 2 : EDGE + 3, :], g_ref[l, EDGE : EDGE + 1, :]
        )
        vy = with_y(
            ty_ref.at[l, 1], v, g_ref[l, EDGE + 3 : EDGE + 4, :], g_ref[l, EDGE + 1 : EDGE + 2, :]
        )
        new_u, new_v = next_currents(
            u, v, ux, uy, vx, vy, open_x(wet_of(wx_ref, l))[:, :W], open_y(wet_of(wy_ref, l))[:R],
            coriolis,
        )
        cur_ref[0, l] = new_u
        cur_ref[1, l] = new_v
        return carry

    lax.fori_loop(0, NL, level, 0, unroll=UNROLL)
    own = ids_ref[0]
    temp = temp_ref[0]
    tx = jnp.concatenate([temp, aside(xh_ref[...], 127 - 104)], 1)
    ty = with_y(ty_ref.at[0, 0], temp, his_ref[52:53, :], los_ref[52:53, :])
    tadv_ref[...] = (
        temp - upwind(tx, east_ref[own], rx)[:, :W] - upwind(ty, north_ref[own], ry)[:R]
    )


def rest_two(
    ids_ref, cur_ref, east_ref, north_ref, wx_ref, wy_ref, temp_ref, xh_ref, los_ref, his_ref,
    out_ref, tadv_ref, ty_ref,
):
    own = ids_ref[0]
    temp = temp_ref[...]
    tx = jnp.concatenate([temp, aside(xh_ref[...], 127 - 108)], 1)
    ty = with_y(ty_ref.at[0, 0], temp, his_ref[58:59, :], los_ref[58:59, :])
    tadv_ref[...] = (
        temp - upwind(tx, east_ref[own], rx)[:, :W] - upwind(ty, north_ref[own], ry)[:R]
    )
    u = cur_ref[0, own]
    v = cur_ref[1, own]
    ux = jnp.concatenate([u, aside(xh_ref[...], 127 - 104)], 1)
    vx = jnp.concatenate([v, aside(xh_ref[...], 127 - 106)], 1)
    uy = with_y(ty_ref.at[1, 0], u, his_ref[56:57, :], los_ref[56:57, :])
    vy = with_y(ty_ref.at[1, 1], v, his_ref[57:58, :], los_ref[57:58, :])
    new_u, new_v = next_currents(
        u, v, ux, uy, vx, vy, open_x(wet_of(wx_ref, own))[:, :W], open_y(wet_of(wy_ref, own))[:R],
        coriolis_of(ids_ref),
    )
    out_ref[0, 0] = new_u
    out_ref[1, 0] = new_v


def biology(
    ids_ref, rate_ref, mixes, parts, solar_ref, wx_ref, tadv_ref, outs, sum_ref, tau_ref
):
    y = ids_ref[0] & 3
    for k, ref in enumerate(parts):
        sum_ref[pl.ds(2 * ((y + 4 - k) & 3), 2)] = ref[...]
    solar = solar_ref[...]
    sea = wx_ref[0, :, :W]
    depth = wx_ref[1, :, :W]
    mu, mortal, recycle = (rate_ref[t, 0:1, :] for t in range(NT))

    def level(l, tau):
        a = 0.04 + 0.03 * sum_ref[l]
        light = solar * jnp.exp(-tau - 0.5 * a)
        tau_ref[l] = tau
        wet = jnp.where(l.astype(f32) < depth, sea, 0.0)
        n, p, d = mixes[0][l], mixes[1][l], mixes[2][l]
        uptake = mu * (light / (light + 0.3)) * p * n / (jnp.abs(n) + 0.5)
        dead = mortal * p
        back = recycle * d
        outs[0][l] = wet * (n - uptake + back)
        outs[1][l] = wet * (p + uptake - dead)
        outs[2][l] = wet * (d + dead - back)
        return tau + a

    lax.fori_loop(0, NL, level, jnp.zeros((R, W), f32), unroll=2)
    own = ids_ref[0]
    tau = tau_ref[own]
    a = 0.04 + 0.03 * sum_ref[own]
    heat = 0.5 * solar * (jnp.exp(-tau) - jnp.exp(-tau - a))
    wet = jnp.where(own.astype(f32) < depth, sea, 0.0)
    return wet * (tadv_ref[...] + heat)


def biology_pack(
    ids_ref, rate_ref, n_ref, p_ref, d_ref, t0, t1, t2, t3, solar_ref, wx_ref, tadv_ref,
    cur_ref, n_out, p_out, d_out, temp_ref, px_ref, pyu_ref, pyd_ref, sum_ref, tau_ref,
):
    outs = (n_out, p_out, d_out)
    temp = biology(
        ids_ref, rate_ref, (n_ref, p_ref, d_ref), (t0, t1, t2, t3), solar_ref, wx_ref, tadv_ref,
        outs, sum_ref, tau_ref,
    )
    temp_ref[...] = temp
    px_ref[...] = jnp.zeros_like(px_ref)
    pyu_ref[...] = jnp.zeros_like(pyu_ref)
    pyd_ref[...] = jnp.zeros_like(pyd_ref)
    pack_tracers(outs, px_ref, pyu_ref, pyd_ref)
    acc = px_ref[...]
    at = lanes(acc.shape)
    for l in range(NL):
        acc = jnp.where(at == 96 + l, pltpu.roll(cur_ref[0, l], 97 + l, 1), acc)
        pyu_ref[48 + l : 49 + l, :] = cur_ref[1, l, R - 1 : R, :]
    own = ids_ref[0]
    for j, value in enumerate((cur_ref[0, own], cur_ref[1, own], temp)):
        acc = put_x(acc, value, 104 + 2 * j, 2)
        pack_rows(value, 56 + j, pyu_ref, pyd_ref)
    px_ref[...] = acc


def biology_last(
    ids_ref, rate_ref, n_ref, p_ref, d_ref, t0, t1, t2, t3, solar_ref, wx_ref, tadv_ref,
    c_ref, temp_ref, sum_ref, tau_ref,
):
    temp_ref[0] = biology(
        ids_ref, rate_ref, (n_ref, p_ref, d_ref), (t0, t1, t2, t3), solar_ref, wx_ref, tadv_ref,
        [c_ref.at[t] for t in range(NT)], sum_ref, tau_ref,
    )


def ring_x(value):
    n, m = lax.axis_size("gx"), lax.axis_size("tracer")
    ahead = [
        (g * m + t, (g + 1) * m + t if g + 1 < n else t ^ (m // 2))
        for g in range(n)
        for t in range(m)
    ]
    back = [(b, a) for a, b in ahead]
    axes = ("gx", "tracer")
    return lax.ppermute(value, axes, ahead), lax.ppermute(value, axes, back)


def ring_y(up, down):
    n = lax.axis_size("gy")
    ahead = [(i, (i + 1) % n) for i in range(n)]
    back = [(b, a) for a, b in ahead]
    return lax.ppermute(up, "gy", ahead), lax.ppermute(down, "gy", back)


def by_y(k):
    return [(z * 4 + y, z * 4 + (y + k) % 4) for z in range(2) for y in range(4)]


def over_z(value):
    return lax.ppermute(value, "tracer", [(i, i ^ 4) for i in range(8)])


def spread_y(value):
    return [value] + [lax.ppermute(value, "tracer", by_y(k)) for k in (1, 2, 3)]


def add_parts(*refs):
    ins, out = refs[:-2], refs[-1]
    acc = ins[0][...] + ins[1][...]
    if len(ins) > 2:
        acc = acc + (ins[2][...] + ins[3][...])
    out[...] = acc


def total(parts, during_y, during_z):
    got = [parts[0]] + [lax.ppermute(parts[k], "tracer", by_y(k)) for k in (1, 2, 3)]
    part = parts[0].shape
    (mine,) = call(add_parts, "add_y", [part], 0, n_any=1)(*got, during_y)
    away = over_z(mine)
    (full,) = call(add_parts, "add_z", [part], 0, n_any=1)(mine, away, during_z)
    return spread_y(full)


def per_device(c, flow, temp, dif, solar, rates, sea, floor):
    ids = jnp.stack(
        [
            lax.axis_index("tracer"),
            lax.axis_index("gx"),
            lax.axis_index("gy"),
            jnp.int32(lax.axis_size("gy")),
            jnp.int32(lax.axis_size("gx")),
        ]
    )
    tile = (R, W)
    col = (NL, R, W)
    part = (2, R, W)
    wide = (NL, R, 2 * W)
    tall = (NL, R + HY, W)
    wets = [(2, R, 2 * W), (2, R + HY, W)]
    two = (NL, 2, R + HY, W)
    other = over_z(flow)
    px, pyu, pyd = call(
        first_pack, "pack_one", [tile, tile, tile], 0,
        [(NT, NL, R, W), (2, 1, R, W), (1, R, W), pltpu.VMEM(tile, jnp.int32),
         pltpu.VMEM(tile, jnp.int32)],
        n_any=5, sems=5,
    )(c, flow, temp, sea, floor)
    px, pyu, pyd = call(pack_other, "pack_two", [tile, tile, tile], 0)(other, px, pyu, pyd)
    left, right = ring_x(px)
    lo, hi = ring_y(pyu, pyd)
    ext, xh, los, his = call(extend_flow, "extend", [(2, 2 * R + 8, W), tile, tile, tile], 1)(
        ids, flow, other, left, right, lo, hi
    )
    gathered = spread_y(ext)
    plank, a0, a1, a2, a3, g, gcol, east, north, wx, wy = call(
        plankton_one, "plankton_one",
        [col, part, part, part, part, (NL, 2 * R + 8, W), tile, wide, tall] + wets, 1,
        [tall, col, tall],
    )(ids, c, *gathered, xh, los, his, dif, sea, floor)
    nutri, detri = (
        call(other_tracer(t), "other_one", [col], 0, [tall, col])(
            c, xh, los, his, east, north, dif, wx
        )[0]
        for t in (0, 2)
    )
    cur, tadv, sun, pace = call(
        rest_one, "rest_one", [(2, NL, R, W), tile, tile, (NT, 8, W)], 2, [two]
    )(
        ids, rates, g, gcol, east, north, wx, wy, temp, xh, los, his, solar
    )
    sums = total((a0, a1, a2, a3), nutri, detri)
    n, p, d, heated, px, pyu, pyd = call(
        biology_pack, "biology_one", [col, col, col, tile, tile, tile, tile], 1, [col, col]
    )(ids, pace, nutri, plank, detri, *sums, sun, wx, tadv, cur)
    left, right = ring_x(px)
    lo, hi = ring_y(pyu, pyd)
    plank, a0, a1, a2, a3, xh, los, his, east, north = call(
        plankton_two, "plankton_two",
        [col, part, part, part, part, tile, tile, tile, wide, tall], 1,
        [tall, col, tall],
    )(ids, p, cur, left, right, lo, hi, dif, wx, wy)
    nutri, detri = (
        call(other_tracer(t), "other_two", [col], 0, [tall, col])(
            q, xh, los, his, east, north, dif, wx
        )[0]
        for t, q in ((0, n), (2, d))
    )
    currents, tadv = call(rest_two, "rest_two", [(2, 1, R, W), tile], 1, [two])(
        ids, cur, east, north, wx, wy, heated, xh, los, his
    )
    sums = total((a0, a1, a2, a3), nutri, detri)
    c, last_temp = call(
        biology_last, "biology_two", [(NT, NL, R, W), (1, R, W)], 1, [col, col]
    )(ids, pace, nutri, plank, detri, *sums, sun, wx, tadv)
    return c, currents, last_temp


def solution(mesh):
    in_specs = (
        P("tracer", None, "gy", "gx"),
        P(None, "tracer", "gy", "gx"),
        P("tracer", "gy", "gx"),
        P(None, "gy", "gx"),
        P("gy", "gx"),
        P("tracer"),
        P("gy", "gx"),
        P("gy", "gx"),
    )
    out_specs = (
        P("tracer", None, "gy", "gx"),
        P(None, "tracer", "gy", "gx"),
        P("tracer", "gy", "gx"),
    )
    return jax.shard_map(
        per_device, mesh=mesh, in_specs=in_specs, out_specs=out_specs, check_vma=False
    )
```

```python
import jax
import jax.numpy as jnp
from jax import lax
from jax.experimental import pallas as pl
from jax.experimental.pallas import tpu as pltpu
from jax.sharding import PartitionSpec as P

NL = 8
R = 64
W = 128
NT = 3
NCH = NT * NL
HY = 8
UNROLL = 4
f32 = jnp.float32
VM = pl.BlockSpec(memory_space=pltpu.VMEM)
AN = pl.BlockSpec(memory_space=pl.ANY)
SM = pl.BlockSpec(memory_space=pltpu.SMEM)


def call(body, name, outs, n_scalar, scratch=(), n_any=0, cost=None):
    def run(*args):
        return pl.pallas_call(
            body,
            name=name,
            out_shape=[jax.ShapeDtypeStruct(s, f32) for s in outs],
            in_specs=[SM] * n_scalar + [VM] * (len(args) - n_scalar - n_any) + [AN] * n_any,
            out_specs=[VM] * len(outs),
            scratch_shapes=[pltpu.VMEM(s, f32) for s in scratch],
            cost_estimate=cost,
            compiler_params=pltpu.CompilerParams(vmem_limit_bytes=40 * 2**20),
        )(*args)

    return run


def lanes(shape):
    return lax.broadcasted_iota(jnp.int32, shape, 1)


def rx(v, k):
    return pltpu.roll(v, k % v.shape[1], 1)


def ry(v, k):
    return pltpu.roll(v, k % v.shape[0], 0)


def aside(v, shift):
    return pltpu.roll(v, shift, 1)


def minmod(a, b):
    return jnp.maximum(jnp.minimum(a, b), 0.0) + jnp.minimum(jnp.maximum(a, b), 0.0)


def coefs(vel):
    up = jnp.maximum(vel, 0.0)
    um = jnp.minimum(vel, 0.0)
    return up, um, 0.5 * up * (1.0 - up), 0.5 * um * (1.0 + um)


def divergence(c, co, roll):
    up, um, a, b = co
    ahead = roll(c, -1)
    d = ahead - c
    s = minmod(d, roll(d, 1))
    flux = up * c + a * s + um * ahead - b * roll(s, -1)
    return flux - roll(flux, 1)


def upwind(c, vel, roll):
    flux = jnp.maximum(vel, 0.0) * c + jnp.minimum(vel, 0.0) * roll(c, -1)
    return flux - roll(flux, 1)


M = 4
ER = R + HY
EW = 2 * W
TILES = 3
NROW = 176
CORNER = 160
FLOW, TEMP, SEA, FLOOR, SUN, DIF = 24, 28, 29, 30, 31, 32
GROWS = 32
COVER = 16 * 2**20
PART = 2 * R + 16


def put_x(px_ref, value, i):
    tile, lane = i >> 4, (i & 15) * 8
    acc = px_ref[tile]
    at = lanes(acc.shape)
    moved = pltpu.roll(value, lane + M, 1)
    px_ref[tile] = jnp.where((at >= lane) & (at < lane + 8), moved, acc)


def put_y(value_ref, index, i, pyu_ref, pyd_ref):
    pyu_ref[pl.ds(4 * i, M), :] = value_ref[index + (slice(R - M, R),)]
    pyd_ref[pl.ds(4 * i, M), :] = value_ref[index + (slice(0, M),)]


def flow_pack(flow_ref, px_ref, pyu_ref, pyd_ref):
    px_ref[...] = jnp.zeros_like(px_ref)
    pyu_ref[...] = jnp.zeros_like(pyu_ref)
    pyd_ref[...] = jnp.zeros_like(pyd_ref)
    for q in range(2):
        put_x(px_ref, flow_ref[q, 0], FLOW + q)
        put_y(flow_ref, (q, 0), FLOW + q, pyu_ref, pyd_ref)


def first_pack(
    c_ref, temp_ref, sea_ref, floor_ref, sun_ref, dif_ref, px_in, pyu_in, pyd_in,
    px_ref, pyu_ref, pyd_ref, mask_ref,
):
    px_ref[...] = px_in[...]
    pyu_ref[...] = pyu_in[...]
    pyd_ref[...] = pyd_in[...]
    mask_ref[0] = sea_ref[...].astype(f32)
    mask_ref[1] = floor_ref[...].astype(f32)
    mask_ref[2] = sun_ref[...]
    mask_ref[3] = temp_ref[0]
    for t in range(NT):
        for l in range(NL):
            put_x(px_ref, c_ref[t, l], t * NL + l)
            put_y(c_ref, (t, l), t * NL + l, pyu_ref, pyd_ref)
    for l in range(NL):
        put_x(px_ref, dif_ref[l], DIF + l)
        put_y(dif_ref, (l,), DIF + l, pyu_ref, pyd_ref)
    for j, i in enumerate((SEA, FLOOR, SUN, TEMP)):
        put_x(px_ref, mask_ref[j], i)
        put_y(mask_ref, (j,), i, pyu_ref, pyd_ref)


def pack_other(flow_ref, other_ref, px_in, px_ref, pair_ref):
    px_ref[...] = px_in[...]
    for q in range(2):
        put_x(px_ref, other_ref[q, 0], FLOW + 2 + q)
        pair_ref[0, q * R : (q + 1) * R, :] = flow_ref[q, 0]
        pair_ref[1, q * R : (q + 1) * R, :] = other_ref[q, 0]


def pack_y(ids_ref, left_ref, right_ref, other_ref, pyu_in, pyd_in, hx_ref, pyu_ref, pyd_ref):
    at = lanes((R, W))
    gx = ids_ref[1]
    for k in range(TILES):
        left = jnp.where(gx == 0, 0.0, left_ref[k])
        right = jnp.where(gx == ids_ref[4] - 1, 0.0, right_ref[k])
        hx_ref[k] = jnp.where(((at >> 2) & 1) == 0, left, right)
    pyu_ref[...] = pyu_in[...]
    pyd_ref[...] = pyd_in[...]
    for j in range(2):
        put_y(other_ref, (j, 0), FLOW + 2 + j, pyu_ref, pyd_ref)
    for k in range(TILES):
        pyu_ref[CORNER + 4 * k : CORNER + 4 * k + M, :] = hx_ref[k, R - M : R, :]
        pyd_ref[CORNER + 4 * k : CORNER + 4 * k + M, :] = hx_ref[k, 0:M, :]


def extend_flow(
    ids_ref, side_ref, lo_ref, hi_ref, e_ref, hx_ref, los_ref, his_ref
):
    gy = ids_ref[2]
    los_ref[...] = jnp.where(gy == 0, 0.0, lo_ref[...])
    his_ref[...] = jnp.where(gy == ids_ref[3] - 1, 0.0, hi_ref[...])
    for k in range(TILES):
        hx_ref[k, 0:R] = side_ref[k]
        hx_ref[k, R:ER] = jnp.zeros((HY, W), f32)
        hx_ref[k, R : R + M] = his_ref[CORNER + 4 * k : CORNER + 4 * k + M, :]
        hx_ref[k, ER - M : ER] = los_ref[CORNER + 4 * k : CORNER + 4 * k + M, :]
    block = hx_ref[FLOW >> 4]
    turned = jnp.concatenate([block, jnp.zeros((W - ER, W), f32)], 0).T
    for k in range(2):
        for q in range(2):
            i = FLOW + 2 * k + q
            at = 8 * q
            e_ref[k, at : at + M, :] = his_ref[4 * i : 4 * i + M, :]
            e_ref[k, at + M : at + 2 * M, :] = los_ref[4 * i : 4 * i + M, :]
        first = (FLOW & 15) * 8 + 16 * k
        e_ref[k, 16:GROWS, :] = turned[first : first + 16, :]


def place(ref, main, side, hi, lo):
    ref[0:R, 0:W] = main
    ref[:, W:] = side
    ref[R : R + M, 0:W] = hi
    ref[ER - M : ER, 0:W] = lo
    return ref[...]


def channel(ref, main, i, hx_ref, los_ref, his_ref):
    side = pltpu.roll(hx_ref[i >> 4], (W + W - M - (i & 15) * 8) & (W - 1), 1)
    return place(ref, main, side, his_ref[pl.ds(4 * i, M), :], los_ref[pl.ds(4 * i, M), :])


def wet_of(wx_ref, l):
    return jnp.where(l < wx_ref[1], wx_ref[0], 0.0)


def open_x(wet):
    return wet * rx(wet, -1)


def open_y(wet):
    return wet * ry(wet, -1)


def laplace(v):
    return rx(v, -1) + rx(v, 1) + ry(v, -1) + ry(v, 1) - 4.0 * v


def next_currents(u, v, wet, coriolis):
    return (
        open_x(wet) * (u + coriolis * v + 0.2 * laplace(u)),
        open_y(wet) * (v - coriolis * u + 0.2 * laplace(v)),
    )


def coriolis_of(ids_ref):
    at = lax.broadcasted_iota(jnp.int32, (ER, EW), 0)
    row = ids_ref[2] * R + jnp.where(at < R + M, at, at - ER)
    rows = (ids_ref[3] * R).astype(f32)
    return 0.1 + 0.1 * row.astype(f32) / rows


def mix(adv_ref, kv_ref, mix_ref, rows, cols):
    for l in range(NL):
        c = adv_ref[l]
        out = c
        if l + 1 < NL:
            out = out + kv_ref[l, :rows, :cols] * (adv_ref[l + 1] - c)
        if l:
            out = out - kv_ref[l - 1, :rows, :cols] * (c - adv_ref[l - 1])
        mix_ref[l] = out


def wide_step(t, l, c, wet, east, north, hx_ref, los_ref, his_ref, slot_ref):
    c = channel(slot_ref, c, t * NL + l, hx_ref, los_ref, his_ref)
    return wet * (c - divergence(c, coefs(east), rx) - divergence(c, coefs(north), ry))


def plankton_one(
    ids_ref, c_ref, mask_ref, dif_ref, g0, g1, g2, g3, e0, e1, e2, e3, hx_ref, los_ref, his_ref,
    mix_ref, a0, a1, a2, a3, u_ref, v_ref, east_ref, north_ref, wx_ref, kv_ref,
    g_ref, e_ref, gx_ref, slot_ref, adv_ref, cols_ref,
):
    y = ids_ref[0] & 3
    z = ids_ref[0] >> 2
    for k, (ref, edge) in enumerate(((g0, e0), (g1, e1), (g2, e2), (g3, e3))):
        for zz in range(2):
            level = ((z + zz) & 1) * 4 + ((y + 4 - k) & 3)
            g_ref[level] = ref[zz]
            e_ref[level] = edge[zz]
    halos = (hx_ref, los_ref, his_ref)
    for k in range(2):
        channel(wx_ref.at[k], mask_ref[k], SEA + k, *halos)
    gx_ref[...] = jnp.concatenate([e_ref[l, 16:GROWS, :] for l in range(NL)], 0).T[:ER]

    for l in range(NL):
        u = place(
            u_ref.at[l], g_ref[l, 0:R, :], pltpu.roll(gx_ref[...], (W - M - 16 * l) % W, 1),
            e_ref[l, 0:M, :], e_ref[l, M : 2 * M, :],
        )
        v = place(
            v_ref.at[l], g_ref[l, R : 2 * R, :], pltpu.roll(gx_ref[...], (W - M - 8 - 16 * l) % W, 1),
            e_ref[l, 2 * M : 3 * M, :], e_ref[l, 3 * M : 4 * M, :],
        )
        wet = wet_of(wx_ref, float(l))
        east = open_x(wet) * u
        north = open_y(wet) * v
        east_ref[l] = east
        north_ref[l] = north
        adv_ref[l] = wide_step(1, l, c_ref[1, l], wet, east, north, *halos, slot_ref.at[0, l])
        if l + 1 < NL:
            dif = channel(slot_ref.at[1, l], dif_ref[l], DIF + l, *halos)
            kv_ref[l] = dif * wet * wet_of(wx_ref, float(l + 1))
    mix(adv_ref, kv_ref, mix_ref, ER, EW)
    acc = jnp.zeros((R, W), f32)
    at = lanes(acc.shape)
    for l in range(NL):
        moved = pltpu.roll(mix_ref[l, 0:R, W:], 4 * l + 2, 1)
        acc = jnp.where((at >= 4 * l) & (at < 4 * l + 4), moved, acc)
    cols_ref[...] = jnp.concatenate([acc, acc], 0).T
    for k, ref in enumerate((a0, a1, a2, a3)):
        j = (y + k) & 3
        for q in range(2):
            l = 2 * j + q
            ref[q * R : (q + 1) * R, :] = mix_ref[l, 0:R, 0:W]
            ref[2 * R + 4 * q : 2 * R + 4 * q + 2, :] = mix_ref[l, R : R + 2, 0:W]
            ref[2 * R + 4 * q + 2 : 2 * R + 4 * q + 4, :] = mix_ref[l, ER - 2 : ER, 0:W]
        ref[2 * R + 8 : PART, :] = cols_ref[pl.ds(pl.multiple_of(8 * j, 8), 8), :]


def other_one(t):
    def body(
        c_ref, hx_ref, los_ref, his_ref, east_ref, north_ref, kv_ref, wx_ref, mix_ref, slot_ref,
        adv_ref,
    ):
        for l in range(NL):
            adv_ref[l] = wide_step(
                t, l, c_ref[t, l], wet_of(wx_ref, float(l)), east_ref[l], north_ref[l], hx_ref,
                los_ref, his_ref, slot_ref.at[l],
            )
        mix(adv_ref, kv_ref, mix_ref, ER, EW)

    return body


def rest_one(
    ids_ref, rate_ref, mask_ref, u_ref, v_ref, east_ref, north_ref, wx_ref, hx_ref, los_ref, his_ref,
    cur_ref, tadv_ref, sun_ref, pace_ref, slot_ref,
):
    for t in range(NT):
        pace_ref[t] = jnp.full((8, W), rate_ref[t], f32)
    channel(sun_ref, mask_ref[2], SUN, hx_ref, los_ref, his_ref)
    coriolis = coriolis_of(ids_ref)

    def level(l, carry):
        new_u, new_v = next_currents(
            u_ref[l], v_ref[l], wet_of(wx_ref, l.astype(f32)), coriolis
        )
        cur_ref[0, l] = new_u
        cur_ref[1, l] = new_v
        return carry

    lax.fori_loop(0, NL, level, 0, unroll=UNROLL)
    own = ids_ref[0]
    temp = channel(slot_ref, mask_ref[3], TEMP, hx_ref, los_ref, his_ref)
    tadv_ref[...] = temp - upwind(temp, east_ref[own], rx) - upwind(temp, north_ref[own], ry)


def inner_step(c_ref, l, wx_ref, east, north):
    c = c_ref[l, 0:R, 0:W]
    div = divergence(c_ref[l, 0:R, :], coefs(east), rx)[:, :W]
    div = div + divergence(c_ref[l, :, 0:W], coefs(north), ry)[:R]
    return jnp.where(float(l) < wx_ref[1, 0:R, 0:W], wx_ref[0, 0:R, 0:W], 0.0) * (c - div)


def plankton_two(
    ids_ref, c_ref, cur_ref, kv_ref, wx_ref, mix_ref, parts, east_ref, north_ref, adv_ref
):
    for l in range(NL):
        wet = wet_of(wx_ref, float(l))
        east = open_x(wet[:R]) * cur_ref[0, l, 0:R, :]
        north = open_y(wet[:, :W]) * cur_ref[1, l, :, 0:W]
        east_ref[l] = east
        north_ref[l] = north
        adv_ref[l] = inner_step(c_ref, l, wx_ref, east, north)
    mix(adv_ref, kv_ref, mix_ref, R, W)
    y = ids_ref[0] & 3
    for k, ref in enumerate(parts):
        ref[...] = mix_ref[pl.ds(2 * ((y + k) & 3), 2)]


def other_two(c_ref, east_ref, north_ref, kv_ref, wx_ref, mix_ref, adv_ref):
    for l in range(NL):
        adv_ref[l] = inner_step(c_ref, l, wx_ref, east_ref[l], north_ref[l])
    mix(adv_ref, kv_ref, mix_ref, R, W)


def rest_two(ids_ref, cur_ref, east_ref, north_ref, wx_ref, temp_ref, out_ref, tadv_ref):
    own = ids_ref[0]
    temp = temp_ref[0:R, 0:W]
    tadv_ref[...] = (
        temp
        - upwind(temp_ref[0:R, :], east_ref[own], rx)[:, :W]
        - upwind(temp_ref[:, 0:W], north_ref[own], ry)[:R]
    )
    new_u, new_v = next_currents(
        cur_ref[0, own], cur_ref[1, own], wet_of(wx_ref, own.astype(f32)), coriolis_of(ids_ref)
    )
    out_ref[0, 0] = new_u[:R, :W]
    out_ref[1, 0] = new_v[:R, :W]


def biology(ids_ref, rate_ref, mixes, absorb, solar, wx, tadv_ref, outs, tau_ref, a_ref):
    sea, depth = wx
    mu, mortal, recycle = (rate_ref[t, 0:1, 0:1] for t in range(NT))
    tau = jnp.zeros(solar.shape, f32)
    for l in range(NL):
        a = 0.04 + 0.03 * absorb(l)
        light = solar * jnp.exp(-tau - 0.5 * a)
        tau_ref[l] = tau
        a_ref[l] = a
        wet = jnp.where(float(l) < depth, sea, 0.0)
        n, p, d = mixes[0][l], mixes[1][l], mixes[2][l]
        uptake = mu * (light / (light + 0.3)) * p * n / (jnp.abs(n) + 0.5)
        dead = mortal * p
        back = recycle * d
        outs[0][l] = wet * (n - uptake + back)
        outs[1][l] = wet * (p + uptake - dead)
        outs[2][l] = wet * (d + dead - back)
        tau = tau + a
    own = ids_ref[0]
    tau, a = tau_ref[own], a_ref[own]
    heat = 0.5 * solar * (jnp.exp(-tau) - jnp.exp(-tau - a))
    wet = jnp.where(own.astype(f32) < depth, sea, 0.0)
    return wet * (tadv_ref[...] + heat)


def biology_one(
    ids_ref, rate_ref, n_ref, p_ref, d_ref, t0, t1, t2, t3, sun_ref, wx_ref, tadv_ref, cur_ref,
    kv_ref, n_out, p_out, d_out, temp_ref, mix_ref, a0, a1, a2, a3, east_ref, north_ref,
    sum_ref, cols_ref, turn_ref, slot_ref, tau_ref, a_ref, adv_ref,
):
    y = ids_ref[0] & 3
    for k, ref in enumerate((t0, t1, t2, t3)):
        j = (y + 4 - k) & 3
        sum_ref[j] = ref[...]
        cols_ref[pl.ds(pl.multiple_of(8 * j, 8), 8), :] = ref[2 * R + 8 : PART, :]
    turned = jnp.concatenate([cols_ref[...], jnp.zeros((W - 4 * NL, W), f32)], 0).T
    turn_ref[...] = turned[:ER]

    def absorb(l):
        j, q = l // 2, l % 2
        slot = slot_ref.at[l]
        slot[0:R, 0:W] = sum_ref[j, q * R : (q + 1) * R, :]
        slot[:, W:] = pltpu.roll(turn_ref[...], (W - 2 - 4 * l) % W, 1)
        at = 2 * R + 4 * q
        slot[R : R + 2, 0:W] = sum_ref[j, at : at + 2, :]
        slot[ER - 2 : ER, 0:W] = sum_ref[j, at + 2 : at + 4, :]
        return slot[...]

    temp_ref[...] = biology(
        ids_ref, rate_ref, (n_ref, p_ref, d_ref), absorb, sun_ref[...], (wx_ref[0], wx_ref[1]),
        tadv_ref, (n_out, p_out, d_out), tau_ref, a_ref,
    )
    plankton_two(
        ids_ref, p_out, cur_ref, kv_ref, wx_ref, mix_ref, (a0, a1, a2, a3), east_ref, north_ref,
        adv_ref,
    )


def biology_two(
    ids_ref, rate_ref, n_ref, p_ref, d_ref, t0, t1, t2, t3, sun_ref, wx_ref, tadv_ref,
    c_ref, temp_ref, sum_ref, tau_ref, a_ref,
):
    y = ids_ref[0] & 3
    for k, ref in enumerate((t0, t1, t2, t3)):
        sum_ref[pl.ds(2 * ((y + 4 - k) & 3), 2)] = ref[...]
    wx = (wx_ref[0, 0:R, 0:W], wx_ref[1, 0:R, 0:W])
    temp_ref[0] = biology(
        ids_ref, rate_ref, (n_ref, p_ref, d_ref), lambda l: sum_ref[l], sun_ref[0:R, 0:W], wx,
        tadv_ref, [c_ref.at[t] for t in range(NT)], tau_ref, a_ref,
    )


def ring_x(value):
    n, m = lax.axis_size("gx"), lax.axis_size("tracer")
    ahead = [
        (g * m + t, (g + 1) * m + t if g + 1 < n else t ^ (m // 2))
        for g in range(n)
        for t in range(m)
    ]
    back = [(b, a) for a, b in ahead]
    axes = ("gx", "tracer")
    return lax.ppermute(value, axes, ahead), lax.ppermute(value, axes, back)


def ring_y(up, down):
    n = lax.axis_size("gy")
    ahead = [(i, (i + 1) % n) for i in range(n)]
    back = [(b, a) for a, b in ahead]
    return lax.ppermute(up, "gy", ahead), lax.ppermute(down, "gy", back)


def by_y(k):
    return [(z * 4 + y, z * 4 + (y + k) % 4) for z in range(2) for y in range(4)]


def over_z(value):
    return lax.ppermute(value, "tracer", [(i, i ^ 4) for i in range(8)])


def spread_y(value):
    return [value] + [lax.ppermute(value, "tracer", by_y(k)) for k in (1, 2, 3)]


def add_parts(*refs):
    ins, out = refs[:-2], refs[-1]
    acc = ins[0][...] + ins[1][...]
    if len(ins) > 2:
        acc = acc + (ins[2][...] + ins[3][...])
    out[...] = acc


def total(parts, during_y, during_z):
    got = [parts[0]] + [lax.ppermute(parts[k], "tracer", by_y(k)) for k in (1, 2, 3)]
    part = parts[0].shape
    (mine,) = call(add_parts, "add_y", [part], 0, n_any=1)(*got, during_y)
    away = over_z(mine)
    (full,) = call(add_parts, "add_z", [part], 0, n_any=1)(mine, away, during_z)
    return spread_y(full)


def per_device(c, flow, temp, dif, solar, rates, sea, floor):
    ids = jnp.stack(
        [
            lax.axis_index("tracer"),
            lax.axis_index("gx"),
            lax.axis_index("gy"),
            jnp.int32(lax.axis_size("gy")),
            jnp.int32(lax.axis_size("gx")),
        ]
    )
    tile = (R, W)
    col = (NL, R, W)
    ext = (ER, EW)
    deep = (NL, ER, EW)
    other = over_z(flow)
    rows = (NROW, W)
    sides = (TILES, R, W)
    packs = call(
        flow_pack, "pack_flow", [sides, rows, rows], 0,
        cost=pl.CostEstimate(flops=0, transcendentals=0, bytes_accessed=COVER),
    )(flow)
    px, pyu, pyd, masks = call(first_pack, "pack_one", [sides, rows, rows, (4, R, W)], 0)(
        c, temp, sea, floor, solar, dif, *packs
    )
    px, pair = call(pack_other, "pack_two", [sides, (2, 2 * R, W)], 0)(flow, other, px)
    left, right = ring_x(px)
    gathered = spread_y(pair)
    side, pyu, pyd = call(pack_y, "pack_y", [sides, rows, rows], 1)(
        ids, left, right, other, pyu, pyd
    )
    lo, hi = ring_y(pyu, pyd)
    own, hx, los, his = call(
        extend_flow, "extend", [(2, GROWS, W), (TILES, ER, W), rows, rows], 1
    )(ids, side, lo, hi)
    margins = spread_y(own)
    part = (PART, W)
    plank, a0, a1, a2, a3, u, v, east, north, wx, kv = call(
        plankton_one, "plankton_one",
        [deep, part, part, part, part, deep, deep, deep, deep, (2, ER, EW), deep], 1,
        [(NL, 2 * R, W), (NL, GROWS, W), (ER, W), (2, NL, ER, EW), deep, (W, W)],
    )(ids, c, masks, dif, *gathered, *margins, hx, los, his)
    nutri, detri = (
        call(other_one(t), "other_one", [deep], 0, [deep, deep])(
            c, hx, los, his, east, north, kv, wx
        )[0]
        for t in (0, 2)
    )
    cur, tadv, sun, pace = call(
        rest_one, "rest_one", [(2, NL, ER, EW), ext, ext, (NT, 8, W)], 2, [ext]
    )(ids, rates, masks, u, v, east, north, wx, hx, los, his)
    sums = total((a0, a1, a2, a3), nutri, detri)
    half = (2, R, W)
    n, p, d, heated, plank, a0, a1, a2, a3, east, north = call(
        biology_one, "biology_one",
        [deep, deep, deep, ext, col, half, half, half, half, (NL, R, EW), (NL, ER, W)], 1,
        [(4, PART, W), (4 * NL, W), (ER, W), deep, deep, deep, col],
    )(ids, pace, nutri, plank, detri, *sums, sun, wx, tadv, cur, kv)
    nutri, detri = (
        call(other_two, "other_two", [col], 0, [col])(q, east, north, kv, wx)[0] for q in (n, d)
    )
    currents, tadv = call(rest_two, "rest_two", [(2, 1, R, W), tile], 1)(
        ids, cur, east, north, wx, heated
    )
    sums = total((a0, a1, a2, a3), nutri, detri)
    c, last_temp = call(
        biology_two, "biology_two", [(NT, NL, R, W), (1, R, W)], 1, [col, col, col]
    )(ids, pace, nutri, plank, detri, *sums, sun, wx, tadv)
    return c, currents, last_temp


def solution(mesh):
    in_specs = (
        P("tracer", None, "gy", "gx"),
        P(None, "tracer", "gy", "gx"),
        P("tracer", "gy", "gx"),
        P(None, "gy", "gx"),
        P("gy", "gx"),
        P("tracer"),
        P("gy", "gx"),
        P("gy", "gx"),
    )
    out_specs = (
        P("tracer", None, "gy", "gx"),
        P(None, "tracer", "gy", "gx"),
        P("tracer", "gy", "gx"),
    )
    return jax.shard_map(
        per_device, mesh=mesh, in_specs=in_specs, out_specs=out_specs, check_vma=False
    )
```

```python
import jax
import jax.numpy as jnp
from jax import lax
from jax.experimental import pallas as pl
from jax.experimental.pallas import tpu as pltpu
from jax.sharding import PartitionSpec as P

NL = 8
R = 64
W = 128
NT = 3
NCH = NT * NL
HY = 8
UNROLL = 4
f32 = jnp.float32
VM = pl.BlockSpec(memory_space=pltpu.VMEM)
AN = pl.BlockSpec(memory_space=pl.ANY)
SM = pl.BlockSpec(memory_space=pltpu.SMEM)


def call(body, name, outs, n_scalar, scratch=(), n_any=0, cost=None):
    def run(*args):
        return pl.pallas_call(
            body,
            name=name,
            out_shape=[jax.ShapeDtypeStruct(s, f32) for s in outs],
            in_specs=[SM] * n_scalar + [VM] * (len(args) - n_scalar - n_any) + [AN] * n_any,
            out_specs=[VM] * len(outs),
            scratch_shapes=[pltpu.VMEM(s, f32) for s in scratch],
            cost_estimate=cost,
            compiler_params=pltpu.CompilerParams(vmem_limit_bytes=40 * 2**20),
        )(*args)

    return run


def lanes(shape):
    return lax.broadcasted_iota(jnp.int32, shape, 1)


def rx(v, k):
    return pltpu.roll(v, k % v.shape[1], 1)


def ry(v, k):
    return pltpu.roll(v, k % v.shape[0], 0)


def aside(v, shift):
    return pltpu.roll(v, shift, 1)


def minmod(a, b):
    return jnp.maximum(jnp.minimum(a, b), 0.0) + jnp.minimum(jnp.maximum(a, b), 0.0)


def coefs(vel):
    up = jnp.maximum(vel, 0.0)
    um = jnp.minimum(vel, 0.0)
    return up, um, 0.5 * up * (1.0 - up), 0.5 * um * (1.0 + um)


def divergence(c, co, roll):
    up, um, a, b = co
    ahead = roll(c, -1)
    d = ahead - c
    s = minmod(d, roll(d, 1))
    flux = up * c + a * s + um * ahead - b * roll(s, -1)
    return flux - roll(flux, 1)


def upwind(c, vel, roll):
    flux = jnp.maximum(vel, 0.0) * c + jnp.minimum(vel, 0.0) * roll(c, -1)
    return flux - roll(flux, 1)


M = 4
ER = R + HY
EW = 2 * W
TILES = 3
NROW = 176
CORNER = 160
FLOW, TEMP, SEA, FLOOR, SUN, DIF = 24, 28, 29, 30, 31, 32
GROWS = 32
COVER = 16 * 2**20
PART = 2 * R + 16


def put_x(px_ref, value, i):
    tile, lane = i >> 4, (i & 15) * 8
    acc = px_ref[tile]
    at = lanes(acc.shape)
    moved = pltpu.roll(value, lane + M, 1)
    px_ref[tile] = jnp.where((at >= lane) & (at < lane + 8), moved, acc)


def put_y(value_ref, index, i, pyu_ref, pyd_ref):
    pyu_ref[pl.ds(4 * i, M), :] = value_ref[index + (slice(R - M, R),)]
    pyd_ref[pl.ds(4 * i, M), :] = value_ref[index + (slice(0, M),)]


def flow_pack(flow_ref, px_ref, pyu_ref, pyd_ref):
    px_ref[...] = jnp.zeros_like(px_ref)
    pyu_ref[...] = jnp.zeros_like(pyu_ref)
    pyd_ref[...] = jnp.zeros_like(pyd_ref)
    for q in range(2):
        put_x(px_ref, flow_ref[q, 0], FLOW + q)
        put_y(flow_ref, (q, 0), FLOW + q, pyu_ref, pyd_ref)


def first_pack(
    c_ref, temp_ref, sea_ref, floor_ref, sun_ref, dif_ref, px_in, pyu_in, pyd_in,
    px_ref, pyu_ref, pyd_ref, mask_ref,
):
    px_ref[...] = px_in[...]
    pyu_ref[...] = pyu_in[...]
    pyd_ref[...] = pyd_in[...]
    mask_ref[0] = sea_ref[...].astype(f32)
    mask_ref[1] = floor_ref[...].astype(f32)
    mask_ref[2] = sun_ref[...]
    mask_ref[3] = temp_ref[0]
    for t in range(NT):
        for l in range(NL):
            put_x(px_ref, c_ref[t, l], t * NL + l)
            put_y(c_ref, (t, l), t * NL + l, pyu_ref, pyd_ref)
    for l in range(NL):
        put_x(px_ref, dif_ref[l], DIF + l)
        put_y(dif_ref, (l,), DIF + l, pyu_ref, pyd_ref)
    for j, i in enumerate((SEA, FLOOR, SUN, TEMP)):
        put_x(px_ref, mask_ref[j], i)
        put_y(mask_ref, (j,), i, pyu_ref, pyd_ref)


def pack_other(flow_ref, other_ref, px_in, px_ref, pair_ref):
    px_ref[...] = px_in[...]
    for q in range(2):
        put_x(px_ref, other_ref[q, 0], FLOW + 2 + q)
        pair_ref[0, q * R : (q + 1) * R, :] = flow_ref[q, 0]
        pair_ref[1, q * R : (q + 1) * R, :] = other_ref[q, 0]


def pack_y(ids_ref, left_ref, right_ref, other_ref, pyu_in, pyd_in, hx_ref, pyu_ref, pyd_ref):
    at = lanes((R, W))
    gx = ids_ref[1]
    for k in range(TILES):
        left = jnp.where(gx == 0, 0.0, left_ref[k])
        right = jnp.where(gx == ids_ref[4] - 1, 0.0, right_ref[k])
        hx_ref[k] = jnp.where(((at >> 2) & 1) == 0, left, right)
    pyu_ref[...] = pyu_in[...]
    pyd_ref[...] = pyd_in[...]
    for j in range(2):
        put_y(other_ref, (j, 0), FLOW + 2 + j, pyu_ref, pyd_ref)
    for k in range(TILES):
        pyu_ref[CORNER + 4 * k : CORNER + 4 * k + M, :] = hx_ref[k, R - M : R, :]
        pyd_ref[CORNER + 4 * k : CORNER + 4 * k + M, :] = hx_ref[k, 0:M, :]


def extend_flow(
    ids_ref, side_ref, lo_ref, hi_ref, e_ref, hx_ref, los_ref, his_ref
):
    gy = ids_ref[2]
    los_ref[...] = jnp.where(gy == 0, 0.0, lo_ref[...])
    his_ref[...] = jnp.where(gy == ids_ref[3] - 1, 0.0, hi_ref[...])
    for k in range(TILES):
        hx_ref[k, 0:R] = side_ref[k]
        hx_ref[k, R:ER] = jnp.zeros((HY, W), f32)
        hx_ref[k, R : R + M] = his_ref[CORNER + 4 * k : CORNER + 4 * k + M, :]
        hx_ref[k, ER - M : ER] = los_ref[CORNER + 4 * k : CORNER + 4 * k + M, :]
    block = hx_ref[FLOW >> 4]
    turned = jnp.concatenate([block, jnp.zeros((W - ER, W), f32)], 0).T
    for k in range(2):
        for q in range(2):
            i = FLOW + 2 * k + q
            at = 8 * q
            e_ref[k, at : at + M, :] = his_ref[4 * i : 4 * i + M, :]
            e_ref[k, at + M : at + 2 * M, :] = los_ref[4 * i : 4 * i + M, :]
        first = (FLOW & 15) * 8 + 16 * k
        e_ref[k, 16:GROWS, :] = turned[first : first + 16, :]


def place(ref, main, side, hi, lo):
    ref[0:R, 0:W] = main
    ref[:, W:] = side
    ref[R : R + M, 0:W] = hi
    ref[ER - M : ER, 0:W] = lo
    return ref[...]


def channel(ref, main, i, hx_ref, los_ref, his_ref):
    side = pltpu.roll(hx_ref[i >> 4], (W + W - M - (i & 15) * 8) & (W - 1), 1)
    return place(ref, main, side, his_ref[pl.ds(4 * i, M), :], los_ref[pl.ds(4 * i, M), :])


def wet_of(wx_ref, l):
    return jnp.where(l < wx_ref[1], wx_ref[0], 0.0)


def open_x(wet):
    return wet * rx(wet, -1)


def open_y(wet):
    return wet * ry(wet, -1)


def laplace(v):
    return rx(v, -1) + rx(v, 1) + ry(v, -1) + ry(v, 1) - 4.0 * v


def next_currents(u, v, wet, coriolis):
    return (
        open_x(wet) * (u + coriolis * v + 0.2 * laplace(u)),
        open_y(wet) * (v - coriolis * u + 0.2 * laplace(v)),
    )


def coriolis_of(ids_ref):
    at = lax.broadcasted_iota(jnp.int32, (ER, EW), 0)
    row = ids_ref[2] * R + jnp.where(at < R + M, at, at - ER)
    rows = (ids_ref[3] * R).astype(f32)
    return 0.1 + 0.1 * row.astype(f32) / rows


def mix(adv_ref, kv_ref, mix_ref, rows, cols):
    for l in range(NL):
        c = adv_ref[l]
        out = c
        if l + 1 < NL:
            out = out + kv_ref[l, :rows, :cols] * (adv_ref[l + 1] - c)
        if l:
            out = out - kv_ref[l - 1, :rows, :cols] * (c - adv_ref[l - 1])
        mix_ref[l] = out


def wide_step(t, l, c, wet, east, north, hx_ref, los_ref, his_ref, slot_ref):
    c = channel(slot_ref, c, t * NL + l, hx_ref, los_ref, his_ref)
    return wet * (c - divergence(c, coefs(east), rx) - divergence(c, coefs(north), ry))


def plankton_one(
    ids_ref, c_ref, mask_ref, dif_ref, g0, g1, g2, g3, e0, e1, e2, e3, hx_ref, los_ref, his_ref,
    mix_ref, a0, a1, a2, a3, u_ref, v_ref, east_ref, north_ref, wx_ref, kv_ref,
    g_ref, e_ref, gx_ref, slot_ref, adv_ref, cols_ref,
):
    y = ids_ref[0] & 3
    z = ids_ref[0] >> 2
    for k, (ref, edge) in enumerate(((g0, e0), (g1, e1), (g2, e2), (g3, e3))):
        for zz in range(2):
            level = ((z + zz) & 1) * 4 + ((y + 4 - k) & 3)
            g_ref[level] = ref[zz]
            e_ref[level] = edge[zz]
    halos = (hx_ref, los_ref, his_ref)
    for k in range(2):
        channel(wx_ref.at[k], mask_ref[k], SEA + k, *halos)
    gx_ref[...] = jnp.concatenate([e_ref[l, 16:GROWS, :] for l in range(NL)], 0).T[:ER]

    for l in range(NL):
        u = place(
            u_ref.at[l], g_ref[l, 0:R, :], pltpu.roll(gx_ref[...], (W - M - 16 * l) % W, 1),
            e_ref[l, 0:M, :], e_ref[l, M : 2 * M, :],
        )
        v = place(
            v_ref.at[l], g_ref[l, R : 2 * R, :], pltpu.roll(gx_ref[...], (W - M - 8 - 16 * l) % W, 1),
            e_ref[l, 2 * M : 3 * M, :], e_ref[l, 3 * M : 4 * M, :],
        )
        wet = wet_of(wx_ref, float(l))
        east = open_x(wet) * u
        north = open_y(wet) * v
        east_ref[l] = east
        north_ref[l] = north
        adv_ref[l] = wide_step(1, l, c_ref[1, l], wet, east, north, *halos, slot_ref.at[0, l])
        if l + 1 < NL:
            dif = channel(slot_ref.at[1, l], dif_ref[l], DIF + l, *halos)
            kv_ref[l] = dif * wet * wet_of(wx_ref, float(l + 1))
    mix(adv_ref, kv_ref, mix_ref, ER, EW)
    acc = jnp.zeros((R, W), f32)
    at = lanes(acc.shape)
    for l in range(NL):
        moved = pltpu.roll(mix_ref[l, 0:R, W:], 4 * l + 2, 1)
        acc = jnp.where((at >= 4 * l) & (at < 4 * l + 4), moved, acc)
    cols_ref[...] = jnp.concatenate([acc, acc], 0).T
    for k, ref in enumerate((a0, a1, a2, a3)):
        j = (y + k) & 3
        for q in range(2):
            l = 2 * j + q
            ref[q * R : (q + 1) * R, :] = mix_ref[l, 0:R, 0:W]
            ref[2 * R + 4 * q : 2 * R + 4 * q + 2, :] = mix_ref[l, R : R + 2, 0:W]
            ref[2 * R + 4 * q + 2 : 2 * R + 4 * q + 4, :] = mix_ref[l, ER - 2 : ER, 0:W]
        ref[2 * R + 8 : PART, :] = cols_ref[pl.ds(pl.multiple_of(8 * j, 8), 8), :]


def other_one(t):
    def body(
        c_ref, hx_ref, los_ref, his_ref, east_ref, north_ref, kv_ref, wx_ref, mix_ref, slot_ref,
        adv_ref,
    ):
        for l in range(NL):
            adv_ref[l] = wide_step(
                t, l, c_ref[t, l], wet_of(wx_ref, float(l)), east_ref[l], north_ref[l], hx_ref,
                los_ref, his_ref, slot_ref.at[l],
            )
        mix(adv_ref, kv_ref, mix_ref, ER, EW)

    return body


def rest_one(
    ids_ref, rate_ref, mask_ref, u_ref, v_ref, east_ref, north_ref, wx_ref, hx_ref, los_ref, his_ref,
    cur_ref, tadv_ref, sun_ref, pace_ref, slot_ref,
):
    for t in range(NT):
        pace_ref[t] = jnp.full((8, W), rate_ref[t], f32)
    channel(sun_ref, mask_ref[2], SUN, hx_ref, los_ref, his_ref)
    coriolis = coriolis_of(ids_ref)

    def level(l, carry):
        new_u, new_v = next_currents(
            u_ref[l], v_ref[l], wet_of(wx_ref, l.astype(f32)), coriolis
        )
        cur_ref[0, l] = new_u
        cur_ref[1, l] = new_v
        return carry

    lax.fori_loop(0, NL, level, 0, unroll=UNROLL)
    own = ids_ref[0]
    temp = channel(slot_ref, mask_ref[3], TEMP, hx_ref, los_ref, his_ref)
    tadv_ref[...] = temp - upwind(temp, east_ref[own], rx) - upwind(temp, north_ref[own], ry)


def inner_step(c_ref, l, wx_ref, east, north):
    c = c_ref[l, 0:R, 0:W]
    div = divergence(c_ref[l, 0:R, :], coefs(east), rx)[:, :W]
    div = div + divergence(c_ref[l, :, 0:W], coefs(north), ry)[:R]
    return jnp.where(float(l) < wx_ref[1, 0:R, 0:W], wx_ref[0, 0:R, 0:W], 0.0) * (c - div)


def plankton_two(
    ids_ref, c_ref, cur_ref, kv_ref, wx_ref, mix_ref, parts, east_ref, north_ref, adv_ref
):
    for l in range(NL):
        wet = wet_of(wx_ref, float(l))
        east = open_x(wet[:R]) * cur_ref[0, l, 0:R, :]
        north = open_y(wet[:, :W]) * cur_ref[1, l, :, 0:W]
        east_ref[l] = east
        north_ref[l] = north
        adv_ref[l] = inner_step(c_ref, l, wx_ref, east, north)
    mix(adv_ref, kv_ref, mix_ref, R, W)
    y = ids_ref[0] & 3
    for k, ref in enumerate(parts):
        ref[...] = mix_ref[pl.ds(2 * ((y + k) & 3), 2)]


def other_two(c_ref, east_ref, north_ref, kv_ref, wx_ref, mix_ref, adv_ref):
    for l in range(NL):
        adv_ref[l] = inner_step(c_ref, l, wx_ref, east_ref[l], north_ref[l])
    mix(adv_ref, kv_ref, mix_ref, R, W)


def rest_two(ids_ref, cur_ref, east_ref, north_ref, wx_ref, temp_ref, out_ref, tadv_ref):
    own = ids_ref[0]
    temp = temp_ref[0:R, 0:W]
    tadv_ref[...] = (
        temp
        - upwind(temp_ref[0:R, :], east_ref[own], rx)[:, :W]
        - upwind(temp_ref[:, 0:W], north_ref[own], ry)[:R]
    )
    new_u, new_v = next_currents(
        cur_ref[0, own], cur_ref[1, own], wet_of(wx_ref, own.astype(f32)), coriolis_of(ids_ref)
    )
    out_ref[0, 0] = new_u[:R, :W]
    out_ref[1, 0] = new_v[:R, :W]


def exchanges(rate_ref, n_ref, p_ref, d_ref, grow_ref, n_out, p_out, d_out):
    mu, mortal, recycle = (rate_ref[t, 0:1, 0:1] for t in range(NT))
    for l in range(NL):
        n, p, d = n_ref[l], p_ref[l], d_ref[l]
        dead = mortal * p
        back = recycle * d
        grow_ref[l] = mu * p * n / (jnp.abs(n) + 0.5)
        n_out[l] = n + back
        p_out[l] = p - dead
        d_out[l] = d + dead - back


def biology(ids_ref, mixes, absorb, solar, wx, tadv_ref, outs, tau_ref, a_ref):
    sea, depth = wx
    tau = jnp.zeros(solar.shape, f32)
    for l in range(NL):
        a = 0.04 + 0.03 * absorb(l)
        light = solar * jnp.exp(-tau - 0.5 * a)
        tau_ref[l] = tau
        a_ref[l] = a
        wet = jnp.where(float(l) < depth, sea, 0.0)
        uptake = light / (light + 0.3) * mixes[0][l]
        outs[0][l] = wet * (mixes[1][l] - uptake)
        outs[1][l] = wet * (mixes[2][l] + uptake)
        outs[2][l] = wet * mixes[3][l]
        tau = tau + a
    own = ids_ref[0]
    tau, a = tau_ref[own], a_ref[own]
    heat = 0.5 * solar * (jnp.exp(-tau) - jnp.exp(-tau - a))
    wet = jnp.where(own.astype(f32) < depth, sea, 0.0)
    return wet * (tadv_ref[...] + heat)


def biology_one(
    ids_ref, grow_ref, n_ref, p_ref, d_ref, t0, t1, t2, t3, sun_ref, wx_ref, tadv_ref, cur_ref,
    kv_ref, n_out, p_out, d_out, temp_ref, mix_ref, a0, a1, a2, a3, east_ref, north_ref,
    sum_ref, cols_ref, turn_ref, slot_ref, tau_ref, a_ref, adv_ref,
):
    y = ids_ref[0] & 3
    for k, ref in enumerate((t0, t1, t2, t3)):
        j = (y + 4 - k) & 3
        sum_ref[j] = ref[...]
        cols_ref[pl.ds(pl.multiple_of(8 * j, 8), 8), :] = ref[2 * R + 8 : PART, :]
    turned = jnp.concatenate([cols_ref[...], jnp.zeros((W - 4 * NL, W), f32)], 0).T
    turn_ref[...] = turned[:ER]

    def absorb(l):
        j, q = l // 2, l % 2
        slot = slot_ref.at[l]
        slot[0:R, 0:W] = sum_ref[j, q * R : (q + 1) * R, :]
        slot[:, W:] = pltpu.roll(turn_ref[...], (W - 2 - 4 * l) % W, 1)
        at = 2 * R + 4 * q
        slot[R : R + 2, 0:W] = sum_ref[j, at : at + 2, :]
        slot[ER - 2 : ER, 0:W] = sum_ref[j, at + 2 : at + 4, :]
        return slot[...]

    temp_ref[...] = biology(
        ids_ref, (grow_ref, n_ref, p_ref, d_ref), absorb, sun_ref[...], (wx_ref[0], wx_ref[1]),
        tadv_ref, (n_out, p_out, d_out), tau_ref, a_ref,
    )
    plankton_two(
        ids_ref, p_out, cur_ref, kv_ref, wx_ref, mix_ref, (a0, a1, a2, a3), east_ref, north_ref,
        adv_ref,
    )


def biology_two(
    ids_ref, grow_ref, n_ref, p_ref, d_ref, t0, t1, t2, t3, sun_ref, wx_ref, tadv_ref,
    c_ref, temp_ref, sum_ref, tau_ref, a_ref,
):
    y = ids_ref[0] & 3
    for k, ref in enumerate((t0, t1, t2, t3)):
        sum_ref[pl.ds(2 * ((y + 4 - k) & 3), 2)] = ref[...]
    wx = (wx_ref[0, 0:R, 0:W], wx_ref[1, 0:R, 0:W])
    temp_ref[0] = biology(
        ids_ref, (grow_ref, n_ref, p_ref, d_ref), lambda l: sum_ref[l], sun_ref[0:R, 0:W], wx,
        tadv_ref, [c_ref.at[t] for t in range(NT)], tau_ref, a_ref,
    )


def ring_x(value):
    n, m = lax.axis_size("gx"), lax.axis_size("tracer")
    ahead = [
        (g * m + t, (g + 1) * m + t if g + 1 < n else t ^ (m // 2))
        for g in range(n)
        for t in range(m)
    ]
    back = [(b, a) for a, b in ahead]
    axes = ("gx", "tracer")
    return lax.ppermute(value, axes, ahead), lax.ppermute(value, axes, back)


def ring_y(up, down):
    n = lax.axis_size("gy")
    ahead = [(i, (i + 1) % n) for i in range(n)]
    back = [(b, a) for a, b in ahead]
    return lax.ppermute(up, "gy", ahead), lax.ppermute(down, "gy", back)


def by_y(k):
    return [(z * 4 + y, z * 4 + (y + k) % 4) for z in range(2) for y in range(4)]


def over_z(value):
    return lax.ppermute(value, "tracer", [(i, i ^ 4) for i in range(8)])


def spread_y(value):
    return [value] + [lax.ppermute(value, "tracer", by_y(k)) for k in (1, 2, 3)]


def add_parts(*refs):
    ins, out = refs[:-2], refs[-1]
    acc = ins[0][...] + ins[1][...]
    if len(ins) > 2:
        acc = acc + (ins[2][...] + ins[3][...])
    out[...] = acc


def total(parts, during_y, during_z):
    got = [parts[0]] + [lax.ppermute(parts[k], "tracer", by_y(k)) for k in (1, 2, 3)]
    part = parts[0].shape
    (mine,) = call(add_parts, "add_y", [part], 0, n_any=1)(*got, during_y)
    away = over_z(mine)
    (full,) = call(add_parts, "add_z", [part], 0, n_any=1)(mine, away, during_z)
    return spread_y(full)


def per_device(c, flow, temp, dif, solar, rates, sea, floor):
    ids = jnp.stack(
        [
            lax.axis_index("tracer"),
            lax.axis_index("gx"),
            lax.axis_index("gy"),
            jnp.int32(lax.axis_size("gy")),
            jnp.int32(lax.axis_size("gx")),
        ]
    )
    tile = (R, W)
    col = (NL, R, W)
    ext = (ER, EW)
    deep = (NL, ER, EW)
    other = over_z(flow)
    rows = (NROW, W)
    sides = (TILES, R, W)
    packs = call(
        flow_pack, "pack_flow", [sides, rows, rows], 0,
        cost=pl.CostEstimate(flops=0, transcendentals=0, bytes_accessed=COVER),
    )(flow)
    px, pyu, pyd, masks = call(first_pack, "pack_one", [sides, rows, rows, (4, R, W)], 0)(
        c, temp, sea, floor, solar, dif, *packs
    )
    px, pair = call(pack_other, "pack_two", [sides, (2, 2 * R, W)], 0)(flow, other, px)
    left, right = ring_x(px)
    gathered = spread_y(pair)
    side, pyu, pyd = call(pack_y, "pack_y", [sides, rows, rows], 1)(
        ids, left, right, other, pyu, pyd
    )
    lo, hi = ring_y(pyu, pyd)
    own, hx, los, his = call(
        extend_flow, "extend", [(2, GROWS, W), (TILES, ER, W), rows, rows], 1
    )(ids, side, lo, hi)
    margins = spread_y(own)
    part = (PART, W)
    plank, a0, a1, a2, a3, u, v, east, north, wx, kv = call(
        plankton_one, "plankton_one",
        [deep, part, part, part, part, deep, deep, deep, deep, (2, ER, EW), deep], 1,
        [(NL, 2 * R, W), (NL, GROWS, W), (ER, W), (2, NL, ER, EW), deep, (W, W)],
    )(ids, c, masks, dif, *gathered, *margins, hx, los, his)
    nutri, detri = (
        call(other_one(t), "other_one", [deep], 0, [deep, deep])(
            c, hx, los, his, east, north, kv, wx
        )[0]
        for t in (0, 2)
    )
    cur, tadv, sun, pace = call(
        rest_one, "rest_one", [(2, NL, ER, EW), ext, ext, (NT, 8, W)], 2, [ext]
    )(ids, rates, masks, u, v, east, north, wx, hx, los, his)
    sums = total((a0, a1, a2, a3), nutri, detri)
    ready = call(exchanges, "exchange_one", [deep] * 4, 0)(pace, nutri, plank, detri)
    half = (2, R, W)
    n, p, d, heated, plank, a0, a1, a2, a3, east, north = call(
        biology_one, "biology_one",
        [deep, deep, deep, ext, col, half, half, half, half, (NL, R, EW), (NL, ER, W)], 1,
        [(4, PART, W), (4 * NL, W), (ER, W), deep, deep, deep, col],
    )(ids, *ready, *sums, sun, wx, tadv, cur, kv)
    nutri, detri = (
        call(other_two, "other_two", [col], 0, [col])(q, east, north, kv, wx)[0] for q in (n, d)
    )
    currents, tadv = call(rest_two, "rest_two", [(2, 1, R, W), tile], 1)(
        ids, cur, east, north, wx, heated
    )
    sums = total((a0, a1, a2, a3), nutri, detri)
    ready = call(exchanges, "exchange_two", [col] * 4, 0)(pace, nutri, plank, detri)
    c, last_temp = call(
        biology_two, "biology_two", [(NT, NL, R, W), (1, R, W)], 1, [col, col, col]
    )(ids, *ready, *sums, sun, wx, tadv)
    return c, currents, last_temp


def solution(mesh):
    in_specs = (
        P("tracer", None, "gy", "gx"),
        P(None, "tracer", "gy", "gx"),
        P("tracer", "gy", "gx"),
        P(None, "gy", "gx"),
        P("gy", "gx"),
        P("tracer"),
        P("gy", "gx"),
        P("gy", "gx"),
    )
    out_specs = (
        P("tracer", None, "gy", "gx"),
        P(None, "tracer", "gy", "gx"),
        P("tracer", "gy", "gx"),
    )
    return jax.shard_map(
        per_device, mesh=mesh, in_specs=in_specs, out_specs=out_specs, check_vma=False
    )
```
